32 devices in a mesh: gx: 16 (over z, y, core), gy: 2 (over x).
Axes of the slice: x: 2, y: 2, z: 4, core: 2. Of those that a mesh axis runs over, the one named last changes fastest.
Arguments:
- prognostic_values: float32 [3, 6, 2048, 1024], P(None, None, 'gx', 'gy'), may hold values from -6 to 6
- forcing_host_values: bfloat16 [3, 6, 2048, 1024], P(None, None, 'gx', 'gy'), may hold values from -6 to 6
- strength: float32 [3, 6], replicated, may hold values from 50 to 200
- level_height: float32 [3], replicated, may hold values from 0.2 to 3
- pbl_height: float32 [2048, 1024], P('gx', 'gy'), may hold values from 0.2 to 3
Outputs:
- tendency: bfloat16 [3, 6, 2048, 1024], P(None, None, 'gx', 'gy')
- energy: float32 [3, 6], replicated
The draws below stay inside these ranges and needn't reach their ends.
All inputs are finite; a program needn't handle non-finite values.
Results may differ from the reference program's by a relative error of at most 0.001.
Values sent between devices are 32-bit elements; how exact they have to be, the bound alone decides.
A program may use at most 64 MiB of HBM per device.

```python
import math
import jax
import jax.numpy as jnp
from jax import lax

KX = 32
KY = 32
VARS = 6
LEV = 3
NX = 2048
NY = 1024


def level_of(rng, extent, cuts, low, high):
    def one(dim, shards_of):
        steps = jax.random.uniform(jax.random.fold_in(jax.random.fold_in(rng, 6), dim), (shards_of,), jnp.float32, low / len(cuts), high / len(cuts))
        return jnp.repeat(jnp.exp(steps), extent[dim] // shards_of).reshape((-1,) + (1,) * (len(extent) - dim - 1))

    gain = one(*cuts[0])
    for cut in cuts[1:]:
        gain = gain * one(*cut)
    return gain


def gaussian(own_key, extent, deviation, most, shards=(), dtype=jnp.bfloat16):
    level = level_of(own_key, extent, shards, -0.22, 0.18) if shards else 1.0
    values = jax.random.normal(own_key, extent, jnp.float32) * deviation * level
    return jnp.minimum(jnp.maximum(values, -most), most).astype(dtype)


def setup_inputs(seed: int = 0) -> dict:
    seeds = jax.random.split(jax.random.key(seed), 6)
    prognostic_values = gaussian(seeds[0], (LEV, VARS, NX, NY), 1.0, 6.0, ((2, 16), (3, 2)), jnp.float32)
    forcing_host_values = gaussian(seeds[1], (LEV, VARS, NX, NY), 1.0, 6.0, ((2, 16), (3, 2)))
    strength = jnp.clip(jnp.exp(jax.random.uniform(seeds[2], (LEV, VARS), jnp.float32, math.log(50.0), math.log(200.0))), 50.0, 200.0)
    level_height = jnp.clip(jax.random.uniform(seeds[3], (LEV,), jnp.float32, 0.2, 3.0), 0.2, 3.0)
    pbl_height = jnp.clip(0.2 + 2.8 * jax.random.uniform(seeds[4], (NX, NY), jnp.float32) ** level_of(seeds[4], (NX, NY), ((0, 16), (1, 2)), -0.2, 0.2), 0.2, 3.0)
    return {"prognostic_values": prognostic_values, "forcing_host_values": forcing_host_values, "strength": strength, "level_height": level_height, "pbl_height": pbl_height}


ramp_depth = 0.25

def cosine_table(total, modes, start, count):
    index = (start + jnp.arange(count)).astype(jnp.float32)
    waves = jnp.arange(modes).astype(jnp.float32)
    scales = jnp.where(waves == 0.0, jnp.sqrt(1.0 / total), jnp.sqrt(2.0 / total)).astype(jnp.float32)
    return scales[None, :] * jnp.cos(jnp.pi * (index[:, None] + 0.5) * waves[None, :] / total)

def reference(prognostic_values, forcing_host_values, strength, level_height, pbl_height):
    meridional_cosines = cosine_table(NX, KX, 0, NX)
    col_basis = cosine_table(NY, KY, 0, NY)
    largest_wavenumber = lax.Precision.HIGHEST

    def one_level(items):
        model, driver, gains, altitude_factor = items
        diff = driver.astype(jnp.float32) - model
        part = jnp.einsum('vij,jb->vib', diff, col_basis, precision=largest_wavenumber)
        mode_factors = jnp.einsum('wl,ywg->ylg', meridional_cosines, part, precision=largest_wavenumber)
        restored_fields = jnp.einsum('ky,jyp->jkp', meridional_cosines, mode_factors, precision=largest_wavenumber)
        recon = jnp.einsum('vib,jb->vij', restored_fields, col_basis, precision=largest_wavenumber)
        damping_share = 1.0 / (1.0 + jnp.exp(-(altitude_factor - pbl_height) / ramp_depth))
        tend = (gains[:, None, None] * damping_share[None] * recon).astype(jnp.bfloat16)
        energy = lax.optimization_barrier(jnp.sum(recon * recon, axis=(1, 2))) / (KX * KY)
        return (tend, energy)
    tendency, energy = lax.map(one_level, (prognostic_values, forcing_host_values, strength, level_height))
    return (tendency, energy)
```

```python
import functools
import math

import jax
import jax.numpy as jnp
from jax import lax
from jax.experimental import pallas as pl
from jax.experimental.pallas import tpu as pltpu
from jax.sharding import PartitionSpec as P

KX = 32
KY = 32
RAMP_DEPTH = 0.25
LANES = 128
SUB = 8
MESH = pl.DeviceIdType.MESH
SPLIT = (4, 7)
FAR = 3

F32 = jnp.float32
BF16 = jnp.bfloat16

SINE = [(-1.0) ** k * (math.pi / 2) ** (2 * k + 1) / math.factorial(2 * k + 1) for k in range(7)]


def basis(total, place, wave):
    turns = (2.0 * place + 1.0) * wave
    rest = turns - (4.0 * total) * jnp.floor(turns * (1.0 / (4.0 * total)))
    t = (jnp.abs(rest - 2.0 * total) - total) * (1.0 / total)
    t2 = t * t
    poly = jnp.full(t.shape, SINE[-1], F32)
    for c in SINE[-2::-1]:
        poly = poly * t2 + c
    scale = jnp.where(wave == 0.0, math.sqrt(1.0 / total), math.sqrt(2.0 / total))
    return scale * (poly * t)


def iota(shape, dim):
    return lax.broadcasted_iota(jnp.int32, shape, dim)


def split(x):
    hi = x.astype(BF16)
    return hi, (x - hi.astype(F32)).astype(BF16)


def group_masks(rows):
    lane = iota((rows, LANES), 1) // KY
    return [lane == g for g in range(LANES // KY)]


def hops(ix, iy):
    return ix // 4 + (ix // 2) % 2 + iy


def plan_owners(gx, gy, fields):
    ends = [(ix, iy) for ix in range(gx) for iy in range(gy) if gx % 2 or ix % 2]
    ends.sort(key=lambda p: hops(*p))
    ends = ends[:max(1, min(fields, len(ends) - 1))]
    extra = [ends[1 + i % (len(ends) - 1)] if len(ends) > 1 else ends[0] for i in range(fields - len(ends))]
    owners = ends[:0:-1] + extra + ends[:1]
    places = [owners[:f].count(owners[f]) for f in range(fields)]
    return owners, places


def plan_slots(fields):
    chunk = 2 if fields % 2 == 0 else 1
    units = fields // chunk
    cuts = [0, units * SPLIT[0] // 9, units * SPLIT[1] // 9, units]
    slots = [range(i * chunk, j * chunk) for i, j in zip(cuts, cuts[1:]) if j > i]
    return slots, chunk


def synthesize(coef, scale, weight_ref, row, col, numbers, variables, put):
    size, cols = coef.shape[0], col.shape[1]
    count = size // SUB
    groups = KX // SUB
    scaled = coef * scale
    stack = jnp.concatenate([jnp.where(m, scaled, 0.0) for m in group_masks(size)], axis=0)
    hi, lo = split(stack)
    lhs = jnp.concatenate([hi, lo, hi], axis=1)
    wave = jnp.dot(lhs, col, preferred_element_type=F32).reshape(groups, count, SUB, cols)
    for k, f in enumerate(numbers):
        whole = jnp.concatenate([wave[g, k] for g in range(groups)], axis=0)
        hi, lo = split(whole)
        rhs = jnp.concatenate([hi, lo, hi, lo], axis=0)
        recon = jnp.dot(row, rhs, preferred_element_type=F32)
        put(k, f, (weight_ref[f // variables] * recon).astype(BF16))


def analysis_kernel(
    dims, prog_hbm, forc_hbm, strength_hbm, level_hbm, pbl_hbm,
    coef_ref, scale_ref, weight_ref, row_ref, col_ref, early_ref,
    strength, level, pbl, prog, forc, part, mine, got, full,
    prog_sem, forc_sem, aux_sem, part_send, part_recv, full_send, full_recv,
):
    gx, gy = dims
    fields, rows, cols = prog.shape
    levels, variables = strength.shape
    groups = KX // SUB
    n_dev = gx * gy
    owners, places = plan_owners(gx, gy, fields)
    slots, chunk = plan_slots(fields)
    n_owned = max(places) + 1
    ix, iy = lax.axis_index("gx"), lax.axis_index("gy")
    me = ix * gy + iy
    far = hops(ix, iy)

    def fetch(c):
        span = pl.ds(c * chunk, chunk)
        return (
            pltpu.make_async_copy(prog_hbm.at[span], prog.at[span], prog_sem.at[c]),
            pltpu.make_async_copy(forc_hbm.at[span], forc.at[span], forc_sem.at[c]),
        )

    for c in range(fields // chunk):
        for copy in fetch(c):
            copy.start()
    aux = [
        pltpu.make_async_copy(pbl_hbm, pbl, aux_sem.at[0]),
        pltpu.make_async_copy(strength_hbm, strength, aux_sem.at[1]),
        pltpu.make_async_copy(level_hbm, level, aux_sem.at[2]),
    ]
    for copy in aux:
        copy.start()

    def owned(f):
        return (ix == owners[f][0]) & (iy == owners[f][1])

    owns = [sum(((owned(f)).astype(jnp.int32) for f in range(fields) if places[f] == k), jnp.int32(0)) for k in range(n_owned)]
    field_at = [
        sum((owned(f).astype(jnp.int32) * f for f in range(fields) if places[f] == k), jnp.int32(0))
        for k in range(n_owned)
    ]

    def each_other(act):
        def body(j, carry):
            t = j + (j >= me).astype(jnp.int32)
            act((t // gy, lax.rem(t, gy)))
            return carry
        if n_dev <= 64:
            for j in range(n_dev - 1):
                body(j, 0)
        else:
            lax.fori_loop(0, n_dev - 1, body, 0)

    barrier = pltpu.get_barrier_semaphore()

    @pl.when(owns[0] > 0)
    def _():
        each_other(lambda t: pl.semaphore_signal(barrier, inc=1, device_id=t, device_id_type=MESH))

    def enter():
        pl.semaphore_wait(barrier, len(set(owners)) - owns[0])

    row = basis(
        rows * gx,
        (ix * rows + iota((KX, rows), 1)).astype(F32),
        iota((KX, rows), 0).astype(F32),
    )
    row_hi, row_lo = split(row)
    row_lhs = jnp.concatenate([row_hi, row_lo], axis=0)
    row_lhs = jnp.concatenate([row_lhs, row_lhs], axis=1)
    col = basis(
        cols * gy,
        (iy * cols + iota((cols, LANES), 0)).astype(F32),
        lax.rem(iota((cols, LANES), 1), KY).astype(F32),
    )
    col_rhs = jnp.concatenate(split(col), axis=1)

    def one_chunk(c, carry):
        for copy in fetch(c):
            copy.wait()
        for k in range(chunk):
            f = c * chunk + k
            diff = forc[f].astype(F32) - prog[f]
            rhs = jnp.concatenate(split(diff), axis=0)
            both = jnp.dot(row_lhs, rhs, preferred_element_type=F32)
            both = both[:KX] + both[KX:]
            for g in range(groups):
                part[g, f] = both[g * SUB:(g + 1) * SUB]
        return carry

    def to_owner(f):
        ox, oy = owners[f]
        at = ox * gy + oy
        return pltpu.make_async_remote_copy(
            src_ref=mine.at[f], dst_ref=got.at[places[f], me - (me > at).astype(jnp.int32)],
            send_sem=part_send.at[f], recv_sem=part_recv.at[places[f]],
            device_id=(ox, oy), device_id_type=MESH,
        )

    def elsewhere(f, act):
        pl.when(jnp.logical_not(owned(f)))(act)

    def to_all(k, f, target):
        return pltpu.make_async_remote_copy(
            src_ref=full.at[f], dst_ref=full.at[f],
            send_sem=full_send.at[k], recv_sem=full_recv.at[f],
            device_id=target, device_id_type=MESH,
        )

    last = len(slots) - 1
    gate = jnp.where(far >= FAR, 0, jnp.where(far > 0, max(last - 1, 0), last))
    for s, numbers in enumerate(slots):
        first, count = numbers[0], len(numbers)
        lax.fori_loop(first // chunk, (first + count) // chunk, one_chunk, 0)
        size = count * SUB
        hi, lo = split(part[:, first:first + count].reshape(groups * size, cols))
        both = jnp.dot(hi, col_rhs, preferred_element_type=F32) + jnp.dot(
            lo, col_rhs, preferred_element_type=F32
        )
        both = both[:, :LANES] + both[:, LANES:]
        coef = both[:size]
        for g, mask in list(enumerate(group_masks(size)))[1:]:
            coef = jnp.where(mask, both[g * size:(g + 1) * size], coef)
        for k, f in enumerate(numbers):
            mine[f] = coef[k * SUB:(k + 1) * SUB]

        @pl.when(gate == s)
        def _(s=s):
            enter()
            for f in range(slots[s][0]):
                elsewhere(f, to_owner(f).start)

        @pl.when(gate <= s)
        def _(numbers=numbers):
            for f in numbers:
                elsewhere(f, to_owner(f).start)

    for copy in aux:
        copy.wait()
    for l in range(levels):
        weight_ref[l] = 1.0 / (1.0 + jnp.exp(-(level[l] - pbl[...]) / RAMP_DEPTH))
        for v in range(variables):
            f = l * variables + v
            scale_ref[f * SUB:(f + 1) * SUB] = jnp.full((SUB, LANES), strength[l, v], F32)
    col_hi, col_lo = split(basis(
        cols * gy,
        (iy * cols + iota((LANES, cols), 1)).astype(F32),
        lax.rem(iota((LANES, cols), 0), KY).astype(F32),
    ))
    col_ref[...] = jnp.concatenate([col_hi, col_hi, col_lo], axis=0)
    row_hi, row_lo = split(basis(
        rows * gx,
        (ix * rows + iota((rows, 4 * KX), 0)).astype(F32),
        lax.rem(iota((rows, 4 * KX), 1), KX).astype(F32),
    ))
    row_ref[...] = jnp.where(
        iota((rows, 4 * KX), 1) < 2 * KX, row_hi.astype(F32), row_lo.astype(F32)
    ).astype(BF16)

    for k in range(n_owned):
        @pl.when(owns[k] > 0)
        def _(k=k):
            f = field_at[k]
            pltpu.make_async_copy(got.at[k], got.at[k], part_recv.at[k]).wait()
            full[f] = mine[f] + jnp.sum(got[k], axis=0)
            each_other(lambda t: to_all(k, f, t).start())

    for s, numbers in enumerate(slots):
        for f in numbers:
            elsewhere(f, to_all(0, f, owners[f]).wait_recv)
            coef_ref[f * SUB:(f + 1) * SUB] = full[f]
        if s < last:
            span = slice(numbers[0] * SUB, (numbers[-1] + 1) * SUB)

            def keep(k, f, value):
                early_ref[f] = value

            synthesize(
                coef_ref[span], scale_ref[span], weight_ref, row_ref[...], col_ref[...],
                numbers, variables, keep,
            )
    for f in range(fields):
        elsewhere(f, to_owner(f).wait_send)
    for k in range(n_owned):
        @pl.when(owns[k] > 0)
        def _(k=k):
            pltpu.make_async_copy(got.at[k], got.at[k], full_send.at[k]).wait()


def synthesis_kernel(
    done, coef_ref, scale_ref, weight_ref, row_ref, col_ref, early_ref, tend_hbm, energy_ref,
    tend, tend_sem,
):
    levels, variables = energy_ref.shape
    fields = levels * variables

    def out(f):
        source = early_ref.at[f] if f < done else tend.at[f - done]
        return pltpu.make_async_copy(
            source, tend_hbm.at[f // variables, f % variables], tend_sem.at[f]
        )

    for f in range(done):
        out(f).start()

    def keep(k, f, value):
        tend[f - done] = value
        if k:
            out(f - 1).start()

    coef = coef_ref[...]
    synthesize(
        coef[done * SUB:], scale_ref[done * SUB:], weight_ref, row_ref[...], col_ref[...],
        range(done, fields), variables, keep,
    )
    out(fields - 1).start()

    power = coef * coef
    at_row = iota((levels, variables), 0)
    at_col = iota((levels, variables), 1)
    energy = jnp.zeros((levels, variables), F32)
    for l in range(levels):
        for v in range(variables):
            f = l * variables + v
            one = jnp.sum(power[f * SUB:(f + 1) * SUB], axis=(0, 1), keepdims=True)
            energy = jnp.where((at_row == l) & (at_col == v), one, energy)
    energy_ref[...] = energy * (1.0 / (KX * KY))

    for f in range(fields):
        out(f).wait()


def per_device(gx, gy, prognostic_values, forcing_host_values, strength, level_height, pbl_height):
    levels, variables, rows, cols = prognostic_values.shape
    fields = levels * variables
    groups = KX // SUB
    n_dev = gx * gy
    slots, chunk = plan_slots(fields)
    n_owned = max(plan_owners(gx, gy, fields)[1]) + 1
    done = slots[-1][0]
    anywhere = pl.BlockSpec(memory_space=pl.ANY)
    vmem = pl.BlockSpec(memory_space=pltpu.VMEM)
    dma = pltpu.SemaphoreType.DMA
    held = pl.pallas_call(
        functools.partial(analysis_kernel, (gx, gy)),
        out_shape=(
            pltpu.VMEM((fields * SUB, LANES), F32),
            pltpu.VMEM((fields * SUB, LANES), F32),
            pltpu.VMEM((levels, rows, cols), F32),
            pltpu.VMEM((rows, 4 * KX), BF16),
            pltpu.VMEM((3 * LANES, cols), BF16),
            pltpu.VMEM((max(done, 1), rows, cols), BF16),
        ),
        in_specs=[anywhere] * 5,
        out_specs=(vmem,) * 6,
        scratch_shapes=[
            pltpu.SMEM((levels, variables), F32),
            pltpu.SMEM((levels,), F32),
            pltpu.VMEM((rows, cols), F32),
            pltpu.VMEM((fields, rows, cols), F32),
            pltpu.VMEM((fields, rows, cols), BF16),
            pltpu.VMEM((groups, fields, SUB, cols), F32),
            pltpu.VMEM((fields, SUB, LANES), F32),
            pltpu.VMEM((n_owned, n_dev - 1, SUB, LANES), F32),
            pltpu.VMEM((fields, SUB, LANES), F32),
            dma((fields // chunk,)),
            dma((fields // chunk,)),
            dma((3,)),
            dma((fields,)),
            dma((n_owned,)),
            dma((n_owned,)),
            dma((fields,)),
        ],
        compiler_params=pltpu.CompilerParams(collective_id=0, has_side_effects=True),
        name="analysis",
    )(
        prognostic_values.reshape(fields, rows, cols),
        forcing_host_values.reshape(fields, rows, cols),
        strength,
        level_height,
        pbl_height,
    )
    tendency, energy = pl.pallas_call(
        functools.partial(synthesis_kernel, done),
        out_shape=(
            jax.ShapeDtypeStruct((levels, variables, rows, cols), BF16),
            jax.ShapeDtypeStruct((levels, variables), F32),
        ),
        in_specs=[vmem] * 6,
        out_specs=(anywhere, vmem),
        scratch_shapes=[
            pltpu.VMEM((fields - done, rows, cols), BF16),
            dma((fields,)),
        ],
        name="synthesis",
    )(*[pltpu.with_memory_space_constraint(x, pltpu.VMEM) for x in held])
    return tendency, energy


def solution(mesh):
    return jax.shard_map(
        functools.partial(per_device, mesh.shape["gx"], mesh.shape["gy"]),
        mesh=mesh,
        in_specs=(P(None, None, "gx", "gy"), P(None, None, "gx", "gy"), P(), P(), P("gx", "gy")),
        out_specs=(P(None, None, "gx", "gy"), P()),
        check_vma=False,
    )
```

```python
import functools
import math

import jax
import jax.numpy as jnp
from jax import lax
from jax.experimental import pallas as pl
from jax.experimental.pallas import tpu as pltpu
from jax.sharding import PartitionSpec as P

KX = 32
KY = 32
RAMP_DEPTH = 0.25
LANES = 128
SUB = 8
MESH = pl.DeviceIdType.MESH
REACH = 3
FAR = 3
TAIL = 1

F32 = jnp.float32
BF16 = jnp.bfloat16

SINE = [(-1.0) ** k * (math.pi / 2) ** (2 * k + 1) / math.factorial(2 * k + 1) for k in range(7)]


def basis(total, place, wave):
    turns = (2.0 * place + 1.0) * wave
    rest = turns - (4.0 * total) * jnp.floor(turns * (1.0 / (4.0 * total)))
    t = (jnp.abs(rest - 2.0 * total) - total) * (1.0 / total)
    t2 = t * t
    poly = jnp.full(t.shape, SINE[-1], F32)
    for c in SINE[-2::-1]:
        poly = poly * t2 + c
    scale = jnp.where(wave == 0.0, math.sqrt(1.0 / total), math.sqrt(2.0 / total))
    return scale * (poly * t)


def iota(shape, dim):
    return lax.broadcasted_iota(jnp.int32, shape, dim)


def split(x):
    hi = x.astype(BF16)
    return hi, (x - hi.astype(F32)).astype(BF16)


def hops(ix, iy):
    return ix // 4 + (ix // 2) % 2 + iy


def plan_groups(fields):
    lanes = LANES // KY
    groups = []
    tile = 0
    for first in range(0, fields, lanes):
        count = min(lanes, fields - first)
        fold = lanes // count
        groups.append((first, count, fold, tile))
        tile += KX // fold // SUB
    return groups, tile


def plan_owners(gx, gy, tiles):
    ends = [(ix, iy) for ix in range(gx) for iy in range(gy) if gx % 2 or ix % 2]
    ends.sort(key=lambda p: hops(*p))
    near = [p for p in ends if hops(*p) <= REACH][:tiles]
    owners = [near[t % len(near)] for t in range(tiles)]
    places = [owners[:t].count(owners[t]) for t in range(tiles)]
    return owners, places


def lane_group(rows):
    return iota((rows, LANES), 1) // KY


def pick(parts, group):
    out = parts[0]
    for i, x in list(enumerate(parts))[1:]:
        out = jnp.where(group == i, x, out)
    return out


def synthesize(coef, count, fold, first, weight_ref, row, col, variables, put):
    group = lane_group(coef.shape[0])
    stack = jnp.concatenate(
        [jnp.where(group == g, coef, 0.0) for g in range(count * fold)], axis=0
    )
    hi, lo = split(stack)
    lhs = jnp.concatenate([hi, lo, hi], axis=1)
    wave = jnp.dot(lhs, col, preferred_element_type=F32)
    for k in range(count):
        f = first + k
        hi, lo = split(wave[k * KX:(k + 1) * KX])
        rhs = jnp.concatenate([hi, lo, hi, lo], axis=0)
        recon = jnp.dot(row, rhs, preferred_element_type=F32)
        put(f, (weight_ref[f // variables] * recon).astype(BF16))


def analysis_kernel(
    dims, prog_hbm, forc_hbm, strength_hbm, level_hbm, pbl_hbm,
    coef_ref, scale_ref, weight_ref, row_ref, col_ref, early_ref,
    strength, level, pbl, prog, forc, part, mine, got, full,
    prog_sem, forc_sem, aux_sem, part_send, part_recv, full_send, full_recv,
):
    gx, gy, tail = dims
    fields, rows, cols = prog.shape
    levels, variables = strength.shape
    n_dev = gx * gy
    groups, tiles = plan_groups(fields)
    owners, places = plan_owners(gx, gy, tiles)
    n_owned = max(places) + 1
    ix, iy = lax.axis_index("gx"), lax.axis_index("gy")
    me = ix * gy + iy
    far = hops(ix, iy)

    def fetch(j):
        first, count = groups[j][:2]
        span = pl.ds(first, count)
        return (
            pltpu.make_async_copy(prog_hbm.at[span], prog.at[span], prog_sem.at[j]),
            pltpu.make_async_copy(forc_hbm.at[span], forc.at[span], forc_sem.at[j]),
        )

    for j in range(len(groups)):
        for copy in fetch(j):
            copy.start()
    aux = [
        pltpu.make_async_copy(pbl_hbm, pbl, aux_sem.at[0]),
        pltpu.make_async_copy(strength_hbm, strength, aux_sem.at[1]),
        pltpu.make_async_copy(level_hbm, level, aux_sem.at[2]),
    ]
    for copy in aux:
        copy.start()

    def owned(t):
        return (ix == owners[t][0]) & (iy == owners[t][1])

    def count_owned(k, weigh):
        return sum(
            (owned(t).astype(jnp.int32) * weigh(t) for t in range(tiles) if places[t] == k),
            jnp.int32(0),
        )

    owns = [count_owned(k, lambda t: 1) for k in range(n_owned)]
    tile_at = [count_owned(k, lambda t: t) for k in range(n_owned)]

    def each_other(act):
        def body(j, carry):
            t = j + (j >= me).astype(jnp.int32)
            act((t // gy, lax.rem(t, gy)))
            return carry
        if n_dev <= 64:
            for j in range(n_dev - 1):
                body(j, 0)
        else:
            lax.fori_loop(0, n_dev - 1, body, 0)

    barrier = pltpu.get_barrier_semaphore()

    @pl.when(owns[0] > 0)
    def _():
        each_other(lambda t: pl.semaphore_signal(barrier, inc=1, device_id=t, device_id_type=MESH))

    def enter():
        pl.semaphore_wait(barrier, len(set(owners)) - owns[0])

    row = basis(
        rows * gx,
        (ix * rows + iota((KX, rows), 1)).astype(F32),
        iota((KX, rows), 0).astype(F32),
    )
    row_hi, row_lo = split(row)
    row_lhs = jnp.concatenate([row_hi, row_lo], axis=0)
    row_lhs = jnp.concatenate([row_lhs, row_lhs], axis=1)
    col = basis(
        cols * gy,
        (iy * cols + iota((cols, LANES), 0)).astype(F32),
        lax.rem(iota((cols, LANES), 1), KY).astype(F32),
    )
    col_rhs = jnp.concatenate(split(col), axis=1)

    def to_owner(t):
        ox, oy = owners[t]
        at = ox * gy + oy
        return pltpu.make_async_remote_copy(
            src_ref=mine.at[t], dst_ref=got.at[places[t], me - (me > at).astype(jnp.int32)],
            send_sem=part_send.at[t], recv_sem=part_recv.at[places[t]],
            device_id=(ox, oy), device_id_type=MESH,
        )

    def elsewhere(t, act):
        pl.when(jnp.logical_not(owned(t)))(act)

    def to_all(k, t, target):
        return pltpu.make_async_remote_copy(
            src_ref=full.at[t], dst_ref=full.at[t],
            send_sem=full_send.at[k], recv_sem=full_recv.at[t],
            device_id=target, device_id_type=MESH,
        )

    def tiles_of(j):
        first, count, fold, tile = groups[j]
        return range(tile, tile + KX // fold // SUB)

    def along_rows(j):
        first, count, fold, tile = groups[j]
        for copy in fetch(j):
            copy.wait()
        for f in range(first, first + count):
            rhs = jnp.concatenate(split(forc[f].astype(F32) - prog[f]), axis=0)
            both = jnp.dot(row_lhs, rhs, preferred_element_type=F32)
            part[f] = both[:KX] + both[KX:]

    def along_cols(j):
        first, count, fold, tile = groups[j]
        hi, lo = split(part[first:first + count].reshape(count * KX, cols))
        both = jnp.dot(hi, col_rhs, preferred_element_type=F32) + jnp.dot(
            lo, col_rhs, preferred_element_type=F32
        )
        both = both[:, :LANES] + both[:, LANES:]
        size = KX // fold
        coef = pick(
            [both[r * size:(r + 1) * size] for r in range(count * fold)], lane_group(size)
        )
        for k, t in enumerate(tiles_of(j)):
            mine[t] = coef[k * SUB:(k + 1) * SUB]

    last = len(groups) - 1
    gate = jnp.where(far >= FAR, 0, jnp.where(far > 0, max(last - 1, 0), last))

    def send(j):
        @pl.when(gate == j)
        def _():
            enter()
            for t in range(tiles_of(j)[0]):
                elsewhere(t, to_owner(t).start)

        @pl.when(gate <= j)
        def _():
            for t in tiles_of(j):
                elsewhere(t, to_owner(t).start)

    for j in range(len(groups)):
        along_rows(j)
        if j:
            along_cols(j - 1)
            send(j - 1)
    along_cols(last)
    send(last)

    for copy in aux:
        copy.wait()
    for l in range(levels):
        weight_ref[l] = 1.0 / (1.0 + jnp.exp(-(level[l] - pbl[...]) / RAMP_DEPTH))
    for j, (first, count, fold, tile) in enumerate(groups):
        scale = pick(
            [
                jnp.full((SUB, LANES), strength[f // variables, f % variables], F32)
                for f in range(first, first + count)
            ],
            lane_group(SUB) // fold,
        )
        for t in tiles_of(j):
            scale_ref[t * SUB:(t + 1) * SUB] = scale
    col_hi, col_lo = split(basis(
        cols * gy,
        (iy * cols + iota((LANES, cols), 1)).astype(F32),
        lax.rem(iota((LANES, cols), 0), KY).astype(F32),
    ))
    col_ref[...] = jnp.concatenate([col_hi, col_hi, col_lo], axis=0)
    row_hi, row_lo = split(basis(
        rows * gx,
        (ix * rows + iota((rows, 4 * KX), 0)).astype(F32),
        lax.rem(iota((rows, 4 * KX), 1), KX).astype(F32),
    ))
    row_ref[...] = jnp.where(
        iota((rows, 4 * KX), 1) < 2 * KX, row_hi.astype(F32), row_lo.astype(F32)
    ).astype(BF16)

    for k in range(n_owned):
        @pl.when(owns[k] > 0)
        def _(k=k):
            t = tile_at[k]
            pltpu.make_async_copy(got.at[k], got.at[k], part_recv.at[k]).wait()
            full[t] = mine[t] + jnp.sum(got[k], axis=0)
            each_other(lambda target: to_all(k, t, target).start())

    for j, (first, count, fold, tile) in enumerate(groups):
        for t in tiles_of(j):
            elsewhere(t, to_all(0, t, owners[t]).wait_recv)
        for t in tiles_of(j):
            coef_ref[t * SUB:(t + 1) * SUB] = full[t]
        if j < len(groups) - tail:
            span = slice(tile * SUB, (tile + len(tiles_of(j))) * SUB)

            def keep(f, value):
                early_ref[f] = value

            synthesize(
                coef_ref[span] * scale_ref[span], count, fold, first,
                weight_ref, row_ref[...], col_ref[...], variables, keep,
            )
    for t in range(tiles):
        elsewhere(t, to_owner(t).wait_send)
    for k in range(n_owned):
        @pl.when(owns[k] > 0)
        def _(k=k):
            pltpu.make_async_copy(got.at[k], got.at[k], full_send.at[k]).wait()


def synthesis_kernel(
    tail, coef_ref, scale_ref, weight_ref, row_ref, col_ref, early_ref, tend_hbm, energy_hbm,
    tend, energy_ref, tend_sem, energy_sem,
):
    levels, variables = energy_ref.shape
    fields = levels * variables
    groups, tiles = plan_groups(fields)
    done = groups[-tail][0]

    def out(f):
        source = early_ref.at[f] if f < done else tend.at[f - done]
        return pltpu.make_async_copy(
            source, tend_hbm.at[f // variables, f % variables], tend_sem.at[f]
        )

    for f in range(done):
        out(f).start()

    def keep(f, value):
        tend[f - done] = value
        if f > done:
            out(f - 1).start()

    for first, count, fold, tile in groups[-tail:]:
        span = slice(tile * SUB, tile * SUB + KX // fold)
        synthesize(
            coef_ref[span] * scale_ref[span], count, fold, first,
            weight_ref, row_ref[...], col_ref[...], variables, keep,
        )
    out(fields - 1).start()

    at_row = iota((levels, variables), 0)
    at_col = iota((levels, variables), 1)
    energy = jnp.zeros((levels, variables), F32)
    for first, count, fold, tile in groups:
        coef = coef_ref[tile * SUB:tile * SUB + KX // fold]
        power = jnp.sum(coef * coef, axis=0, keepdims=True)
        group = lane_group(1) // fold
        for k in range(count):
            f = first + k
            one = jnp.sum(jnp.where(group == k, power, 0.0), axis=(0, 1), keepdims=True)
            energy = jnp.where(
                (at_row == f // variables) & (at_col == f % variables), one, energy
            )
    energy_ref[...] = energy * (1.0 / (KX * KY))
    result = pltpu.make_async_copy(energy_ref, energy_hbm, energy_sem)
    result.start()

    for f in range(fields):
        out(f).wait()
    result.wait()


def per_device(gx, gy, prognostic_values, forcing_host_values, strength, level_height, pbl_height):
    levels, variables, rows, cols = prognostic_values.shape
    fields = levels * variables
    n_dev = gx * gy
    groups, tiles = plan_groups(fields)
    n_owned = max(plan_owners(gx, gy, tiles)[1]) + 1
    tail = min(TAIL, len(groups))
    done = groups[-tail][0]
    anywhere = pl.BlockSpec(memory_space=pl.ANY)
    vmem = pl.BlockSpec(memory_space=pltpu.VMEM)
    dma = pltpu.SemaphoreType.DMA
    held = pl.pallas_call(
        functools.partial(analysis_kernel, (gx, gy, tail)),
        out_shape=(
            pltpu.VMEM((tiles * SUB, LANES), F32),
            pltpu.VMEM((tiles * SUB, LANES), F32),
            pltpu.VMEM((levels, rows, cols), F32),
            pltpu.VMEM((rows, 4 * KX), BF16),
            pltpu.VMEM((3 * LANES, cols), BF16),
            pltpu.VMEM((max(done, 1), rows, cols), BF16),
        ),
        in_specs=[anywhere] * 5,
        out_specs=(vmem,) * 6,
        scratch_shapes=[
            pltpu.SMEM((levels, variables), F32),
            pltpu.SMEM((levels,), F32),
            pltpu.VMEM((rows, cols), F32),
            pltpu.VMEM((fields, rows, cols), F32),
            pltpu.VMEM((fields, rows, cols), BF16),
            pltpu.VMEM((fields, KX, cols), F32),
            pltpu.VMEM((tiles, SUB, LANES), F32),
            pltpu.VMEM((n_owned, n_dev - 1, SUB, LANES), F32),
            pltpu.VMEM((tiles, SUB, LANES), F32),
            dma((len(groups),)),
            dma((len(groups),)),
            dma((3,)),
            dma((tiles,)),
            dma((n_owned,)),
            dma((n_owned,)),
            dma((tiles,)),
        ],
        compiler_params=pltpu.CompilerParams(collective_id=0, has_side_effects=True),
        name="analysis",
    )(
        prognostic_values.reshape(fields, rows, cols),
        forcing_host_values.reshape(fields, rows, cols),
        strength,
        level_height,
        pbl_height,
    )
    tendency, energy = pl.pallas_call(
        functools.partial(synthesis_kernel, tail),
        out_shape=(
            jax.ShapeDtypeStruct((levels, variables, rows, cols), BF16),
            jax.ShapeDtypeStruct((levels, variables), F32),
        ),
        in_specs=[vmem] * 6,
        out_specs=(anywhere, anywhere),
        scratch_shapes=[
            pltpu.VMEM((fields - done, rows, cols), BF16),
            pltpu.VMEM((levels, variables), F32),
            dma((fields,)),
            dma,
        ],
        name="synthesis",
    )(*[pltpu.with_memory_space_constraint(x, pltpu.VMEM) for x in held])
    return tendency, energy


def solution(mesh):
    return jax.shard_map(
        functools.partial(per_device, mesh.shape["gx"], mesh.shape["gy"]),
        mesh=mesh,
        in_specs=(P(None, None, "gx", "gy"), P(None, None, "gx", "gy"), P(), P(), P("gx", "gy")),
        out_specs=(P(None, None, "gx", "gy"), P()),
        check_vma=False,
    )
```

```python
import functools
import math

import jax
import jax.numpy as jnp
from jax import lax
from jax.experimental import pallas as pl
from jax.experimental.pallas import tpu as pltpu
from jax.sharding import PartitionSpec as P

KX = 32
KY = 32
RAMP_DEPTH = 0.25
LANES = 128
SUB = 8
MESH = pl.DeviceIdType.MESH
REACH = 3
FAR = 3
TAIL = 2

F32 = jnp.float32
BF16 = jnp.bfloat16

SINE = [(-1.0) ** k * (math.pi / 2) ** (2 * k + 1) / math.factorial(2 * k + 1) for k in range(7)]


def basis(total, place, wave):
    turns = (2.0 * place + 1.0) * wave
    rest = turns - (4.0 * total) * jnp.floor(turns * (1.0 / (4.0 * total)))
    t = (jnp.abs(rest - 2.0 * total) - total) * (1.0 / total)
    t2 = t * t
    poly = jnp.full(t.shape, SINE[-1], F32)
    for c in SINE[-2::-1]:
        poly = poly * t2 + c
    scale = jnp.where(wave == 0.0, math.sqrt(1.0 / total), math.sqrt(2.0 / total))
    return scale * (poly * t)


def iota(shape, dim):
    return lax.broadcasted_iota(jnp.int32, shape, dim)


def split(x):
    hi = x.astype(BF16)
    return hi, (x - hi.astype(F32)).astype(BF16)


def hops(ix, iy):
    return ix // 4 + (ix // 2) % 2 + iy


def plan_groups(fields):
    lanes = LANES // KY
    groups = []
    tile = 0
    for first in range(0, fields, lanes):
        count = min(lanes, fields - first)
        fold = lanes // count
        groups.append((first, count, fold, tile))
        tile += KX // fold // SUB
    return groups, tile


def plan_owners(gx, gy, tiles):
    ends = [(ix, iy) for ix in range(gx) for iy in range(gy) if gx % 2 or ix % 2]
    ends.sort(key=lambda p: hops(*p))
    near = [p for p in ends if hops(*p) <= REACH][:tiles]
    owners = [near[t % len(near)] for t in range(tiles)]
    places = [owners[:t].count(owners[t]) for t in range(tiles)]
    return owners, places


def lane_group(rows):
    return iota((rows, LANES), 1) // KY


def pick(parts, group):
    out = parts[0]
    for i, x in list(enumerate(parts))[1:]:
        out = jnp.where(group == i, x, out)
    return out


def expand_cols(parts, col):
    stack = []
    for coef, count, fold in parts:
        group = lane_group(coef.shape[0])
        stack.extend(jnp.where(group == g, coef, 0.0) for g in range(count * fold))
    hi, lo = split(jnp.concatenate(stack, axis=0))
    lhs = jnp.concatenate([hi, lo, hi], axis=1)
    return split(jnp.dot(lhs, col, preferred_element_type=F32))


def expand_rows(hi, lo, row, weight):
    rhs = jnp.concatenate([hi, lo, hi, lo], axis=0)
    return (weight * jnp.dot(row, rhs, preferred_element_type=F32)).astype(BF16)


def analysis_kernel(
    dims, prog_hbm, forc_hbm, strength_hbm, level_hbm, pbl_hbm,
    coef_ref, scale_ref, weight_ref, row_ref, col_ref, early_ref,
    strength, level, pbl, prog, forc, part, mine, got, full, wave,
    prog_sem, forc_sem, aux_sem, part_send, part_recv, full_send, full_recv,
):
    gx, gy, tail = dims
    fields, rows, cols = prog.shape
    levels, variables = strength.shape
    n_dev = gx * gy
    groups, tiles = plan_groups(fields)
    owners, places = plan_owners(gx, gy, tiles)
    n_owned = max(places) + 1
    ix, iy = lax.axis_index("gx"), lax.axis_index("gy")
    me = ix * gy + iy
    far = hops(ix, iy)

    def fetch(j):
        first, count = groups[j][:2]
        span = pl.ds(first, count)
        return (
            pltpu.make_async_copy(prog_hbm.at[span], prog.at[span], prog_sem.at[j]),
            pltpu.make_async_copy(forc_hbm.at[span], forc.at[span], forc_sem.at[j]),
        )

    for j in range(len(groups)):
        for copy in fetch(j):
            copy.start()
    aux = [
        pltpu.make_async_copy(pbl_hbm, pbl, aux_sem.at[0]),
        pltpu.make_async_copy(strength_hbm, strength, aux_sem.at[1]),
        pltpu.make_async_copy(level_hbm, level, aux_sem.at[2]),
    ]
    for copy in aux:
        copy.start()

    def tiles_of(j):
        first, count, fold, tile = groups[j]
        return range(tile, tile + KX // fold // SUB)

    def owned(t):
        return (ix == owners[t][0]) & (iy == owners[t][1])

    def count_owned(k, weigh):
        return sum(
            (owned(t).astype(jnp.int32) * weigh(t) for t in range(tiles) if places[t] == k),
            jnp.int32(0),
        )

    group_of = [j for j in range(len(groups)) for t in tiles_of(j)]
    owns = [count_owned(k, lambda t: 1) for k in range(n_owned)]
    tile_at = [count_owned(k, lambda t: t) for k in range(n_owned)]
    group_at = [count_owned(k, lambda t: group_of[t]) for k in range(n_owned)]

    def settle(ref, sem):
        pltpu.make_async_copy(ref, ref, sem).wait()

    def settle_tiles(buf, sem, first, count, own, most):
        for c in range(min(most, count - 1) + 1):
            pl.when(own == c)(lambda c=c: settle(buf.at[pl.ds(first, count - c)], sem))

    def each_other(act):
        def body(j, carry):
            t = j + (j >= me).astype(jnp.int32)
            act((t // gy, lax.rem(t, gy)))
            return carry
        if n_dev <= 64:
            for j in range(n_dev - 1):
                body(j, 0)
        else:
            lax.fori_loop(0, n_dev - 1, body, 0)

    barrier = pltpu.get_barrier_semaphore()

    @pl.when(owns[0] > 0)
    def _():
        each_other(lambda t: pl.semaphore_signal(barrier, inc=1, device_id=t, device_id_type=MESH))

    def enter():
        pl.semaphore_wait(barrier, len(set(owners)) - owns[0])

    row = basis(
        rows * gx,
        (ix * rows + iota((KX, rows), 1)).astype(F32),
        iota((KX, rows), 0).astype(F32),
    )
    row_hi, row_lo = split(row)
    row_lhs = jnp.concatenate([row_hi, row_lo], axis=0)
    row_lhs = jnp.concatenate([row_lhs, row_lhs], axis=1)
    col = basis(
        cols * gy,
        (iy * cols + iota((cols, LANES), 0)).astype(F32),
        lax.rem(iota((cols, LANES), 1), KY).astype(F32),
    )
    col_rhs = jnp.concatenate(split(col), axis=1)

    def to_owner(t):
        ox, oy = owners[t]
        at = ox * gy + oy
        return pltpu.make_async_remote_copy(
            src_ref=mine.at[t], dst_ref=got.at[places[t], me - (me > at).astype(jnp.int32)],
            send_sem=part_send, recv_sem=part_recv.at[places[t]],
            device_id=(ox, oy), device_id_type=MESH,
        )

    def elsewhere(t, act):
        pl.when(jnp.logical_not(owned(t)))(act)

    def to_all(tile, group, target):
        return pltpu.make_async_remote_copy(
            src_ref=full.at[tile], dst_ref=full.at[tile],
            send_sem=full_send, recv_sem=full_recv.at[group],
            device_id=target, device_id_type=MESH,
        )

    def along_rows(j):
        first, count, fold, tile = groups[j]
        for copy in fetch(j):
            copy.wait()
        for f in range(first, first + count):
            rhs = jnp.concatenate(split(forc[f].astype(F32) - prog[f]), axis=0)
            both = jnp.dot(row_lhs, rhs, preferred_element_type=F32)
            part[f] = both[:KX] + both[KX:]

    def along_cols(j):
        first, count, fold, tile = groups[j]
        hi, lo = split(part[first:first + count].reshape(count * KX, cols))
        both = jnp.dot(hi, col_rhs, preferred_element_type=F32) + jnp.dot(
            lo, col_rhs, preferred_element_type=F32
        )
        both = both[:, :LANES] + both[:, LANES:]
        size = KX // fold
        coef = pick(
            [both[r * size:(r + 1) * size] for r in range(count * fold)], lane_group(size)
        )
        for k, t in enumerate(tiles_of(j)):
            mine[t] = coef[k * SUB:(k + 1) * SUB]

    last = len(groups) - 1
    gate = jnp.where(far >= FAR, 0, jnp.where(far > 0, max(last - 1, 0), last))

    def send(j):
        @pl.when(gate == j)
        def _():
            enter()
            for t in range(tiles_of(j)[0]):
                elsewhere(t, to_owner(t).start)

        @pl.when(gate <= j)
        def _():
            for t in tiles_of(j):
                elsewhere(t, to_owner(t).start)

    for j in range(len(groups)):
        along_rows(j)
        if j:
            along_cols(j - 1)
            send(j - 1)
    along_cols(last)
    send(last)

    for copy in aux:
        copy.wait()
    for l in range(levels):
        weight_ref[l] = 1.0 / (1.0 + jnp.exp(-(level[l] - pbl[...]) / RAMP_DEPTH))
    for j, (first, count, fold, tile) in enumerate(groups):
        scale = pick(
            [
                jnp.full((SUB, LANES), strength[f // variables, f % variables], F32)
                for f in range(first, first + count)
            ],
            lane_group(SUB) // fold,
        )
        for t in tiles_of(j):
            scale_ref[t * SUB:(t + 1) * SUB] = scale
    col_hi, col_lo = split(basis(
        cols * gy,
        (iy * cols + iota((LANES, cols), 1)).astype(F32),
        lax.rem(iota((LANES, cols), 0), KY).astype(F32),
    ))
    col_ref[...] = jnp.concatenate([col_hi, col_hi, col_lo], axis=0)
    row_hi, row_lo = split(basis(
        rows * gx,
        (ix * rows + iota((rows, 4 * KX), 0)).astype(F32),
        lax.rem(iota((rows, 4 * KX), 1), KX).astype(F32),
    ))
    row_ref[...] = jnp.where(
        iota((rows, 4 * KX), 1) < 2 * KX, row_hi.astype(F32), row_lo.astype(F32)
    ).astype(BF16)

    for k in range(n_owned):
        @pl.when(owns[k] > 0)
        def _(k=k):
            t = tile_at[k]
            settle(got.at[k], part_recv.at[k])
            full[t] = mine[t] + jnp.sum(got[k], axis=0)
            each_other(lambda target: to_all(t, group_at[k], target).start())

    early = len(groups) - tail

    def widen(j):
        first, count, fold, tile = groups[j]
        span = slice(tile * SUB, tile * SUB + KX // fold)
        hi, lo = expand_cols([(coef_ref[span] * scale_ref[span], count, fold)], col_ref[...])
        wave[j % 2, 0, :count * KX] = hi
        wave[j % 2, 1, :count * KX] = lo

    def finish(j):
        first, count, fold, tile = groups[j]
        for k in range(count):
            f = first + k
            span = slice(k * KX, (k + 1) * KX)
            early_ref[f] = expand_rows(
                wave[j % 2, 0, span], wave[j % 2, 1, span], row_ref[...],
                weight_ref[f // variables],
            )

    for j, (first, count, fold, tile) in enumerate(groups):
        if j == early and j:
            finish(j - 1)
        mine_here = sum((owned(t).astype(jnp.int32) for t in tiles_of(j)), jnp.int32(0))
        held = [owners[t] for t in tiles_of(j)]
        settle_tiles(
            full, full_recv.at[j], tile, len(held), mine_here, max(held.count(o) for o in held)
        )
        for t in tiles_of(j):
            coef_ref[t * SUB:(t + 1) * SUB] = full[t]
        if j < early:
            widen(j)
            if j:
                finish(j - 1)
    settle_tiles(mine, part_send, 0, tiles, sum(owns), n_owned)
    for c in range(1, n_owned + 1):
        pl.when(sum(owns) == c)(lambda c=c: settle(got.at[pl.ds(0, c)], full_send))


def synthesis_kernel(
    tail, coef_ref, scale_ref, weight_ref, row_ref, col_ref, early_ref, tend_hbm, energy_hbm,
    tend, energy_ref, tend_sem, energy_sem,
):
    levels, variables = energy_ref.shape
    fields = levels * variables
    groups, tiles = plan_groups(fields)
    done = groups[-tail][0]

    def out(f):
        source = early_ref.at[f] if f < done else tend.at[f - done]
        return pltpu.make_async_copy(
            source, tend_hbm.at[f // variables, f % variables], tend_sem
        )

    for f in range(done):
        out(f).start()

    at_row = iota((levels, variables), 0)
    at_col = iota((levels, variables), 1)
    energy = jnp.zeros((levels, variables), F32)
    for first, count, fold, tile in groups:
        coef = coef_ref[tile * SUB:tile * SUB + KX // fold]
        power = jnp.sum(coef * coef, axis=0, keepdims=True)
        group = lane_group(1) // fold
        for k in range(count):
            f = first + k
            one = jnp.sum(jnp.where(group == k, power, 0.0), axis=(0, 1), keepdims=True)
            energy = jnp.where(
                (at_row == f // variables) & (at_col == f % variables), one, energy
            )
    energy_ref[...] = energy * (1.0 / (KX * KY))
    result = pltpu.make_async_copy(energy_ref, energy_hbm, energy_sem)
    result.start()

    parts = []
    for first, count, fold, tile in groups[-tail:]:
        span = slice(tile * SUB, tile * SUB + KX // fold)
        parts.append((coef_ref[span] * scale_ref[span], count, fold))
    hi, lo = expand_cols(parts, col_ref[...])
    for f in range(done, fields):
        span = slice((f - done) * KX, (f - done + 1) * KX)
        tend[f - done] = expand_rows(
            hi[span], lo[span], row_ref[...], weight_ref[f // variables]
        )
        if f > done:
            out(f - 1).start()
    out(fields - 1).start()

    pltpu.make_async_copy(tend_hbm, tend_hbm, tend_sem).wait()
    result.wait()


def per_device(gx, gy, prognostic_values, forcing_host_values, strength, level_height, pbl_height):
    levels, variables, rows, cols = prognostic_values.shape
    fields = levels * variables
    n_dev = gx * gy
    groups, tiles = plan_groups(fields)
    n_owned = max(plan_owners(gx, gy, tiles)[1]) + 1
    tail = min(TAIL, len(groups))
    done = groups[-tail][0]
    anywhere = pl.BlockSpec(memory_space=pl.ANY)
    vmem = pl.BlockSpec(memory_space=pltpu.VMEM)
    dma = pltpu.SemaphoreType.DMA
    held = pl.pallas_call(
        functools.partial(analysis_kernel, (gx, gy, tail)),
        out_shape=(
            pltpu.VMEM((tiles * SUB, LANES), F32),
            pltpu.VMEM((tiles * SUB, LANES), F32),
            pltpu.VMEM((levels, rows, cols), F32),
            pltpu.VMEM((rows, 4 * KX), BF16),
            pltpu.VMEM((3 * LANES, cols), BF16),
            pltpu.VMEM((max(done, 1), rows, cols), BF16),
        ),
        in_specs=[anywhere] * 5,
        out_specs=(vmem,) * 6,
        scratch_shapes=[
            pltpu.SMEM((levels, variables), F32),
            pltpu.SMEM((levels,), F32),
            pltpu.VMEM((rows, cols), F32),
            pltpu.VMEM((fields, rows, cols), F32),
            pltpu.VMEM((fields, rows, cols), BF16),
            pltpu.VMEM((fields, KX, cols), F32),
            pltpu.VMEM((tiles, SUB, LANES), F32),
            pltpu.VMEM((n_owned, n_dev - 1, SUB, LANES), F32),
            pltpu.VMEM((tiles, SUB, LANES), F32),
            pltpu.VMEM((2, 2, LANES, cols), BF16),
            dma((len(groups),)),
            dma((len(groups),)),
            dma((3,)),
            dma,
            dma((n_owned,)),
            dma,
            dma((len(groups),)),
        ],
        compiler_params=pltpu.CompilerParams(collective_id=0, has_side_effects=True),
        name="analysis",
    )(
        prognostic_values.reshape(fields, rows, cols),
        forcing_host_values.reshape(fields, rows, cols),
        strength,
        level_height,
        pbl_height,
    )
    tendency, energy = pl.pallas_call(
        functools.partial(synthesis_kernel, tail),
        out_shape=(
            jax.ShapeDtypeStruct((levels, variables, rows, cols), BF16),
            jax.ShapeDtypeStruct((levels, variables), F32),
        ),
        in_specs=[vmem] * 6,
        out_specs=(anywhere, anywhere),
        scratch_shapes=[
            pltpu.VMEM((fields - done, rows, cols), BF16),
            pltpu.VMEM((levels, variables), F32),
            dma,
            dma,
        ],
        name="synthesis",
    )(*[pltpu.with_memory_space_constraint(x, pltpu.VMEM) for x in held])
    return tendency, energy


def solution(mesh):
    return jax.shard_map(
        functools.partial(per_device, mesh.shape["gx"], mesh.shape["gy"]),
        mesh=mesh,
        in_specs=(P(None, None, "gx", "gy"), P(None, None, "gx", "gy"), P(), P(), P("gx", "gy")),
        out_specs=(P(None, None, "gx", "gy"), P()),
        check_vma=False,
    )
```

```python
import functools
import math

import jax
import jax.numpy as jnp
from jax import lax
from jax.experimental import pallas as pl
from jax.experimental.pallas import tpu as pltpu
from jax.sharding import PartitionSpec as P

KX = 32
KY = 32
RAMP_DEPTH = 0.25
LANES = 128
SUB = 8
MESH = pl.DeviceIdType.MESH
REACH = 3
FAR = 3
TAIL = 2
BLOCK = 4

F32 = jnp.float32
BF16 = jnp.bfloat16

SINE = [(-1.0) ** k * (math.pi / 2) ** (2 * k + 1) / math.factorial(2 * k + 1) for k in range(7)]


def basis(total, place, wave):
    turns = (2.0 * place + 1.0) * wave
    rest = turns - (4.0 * total) * jnp.floor(turns * (1.0 / (4.0 * total)))
    t = (jnp.abs(rest - 2.0 * total) - total) * (1.0 / total)
    t2 = t * t
    poly = jnp.full(t.shape, SINE[-1], F32)
    for c in SINE[-2::-1]:
        poly = poly * t2 + c
    scale = jnp.where(wave == 0.0, math.sqrt(1.0 / total), math.sqrt(2.0 / total))
    return scale * (poly * t)


def iota(shape, dim):
    return lax.broadcasted_iota(jnp.int32, shape, dim)


def split(x):
    hi = x.astype(BF16)
    return hi, (x - hi.astype(F32)).astype(BF16)


def hops(ix, iy):
    return ix // 4 + (ix // 2) % 2 + iy


def plan_groups(fields):
    lanes = LANES // KY
    groups = []
    tile = 0
    for first in range(0, fields, lanes):
        count = min(lanes, fields - first)
        fold = lanes // count
        groups.append((first, count, fold, tile))
        tile += KX // fold // SUB
    return groups, tile


def plan_blocks(fields):
    return [range(f, min(f + BLOCK, fields)) for f in range(0, fields, BLOCK)]


def plan_owners(gx, gy, tiles):
    ends = [(ix, iy) for ix in range(gx) for iy in range(gy) if gx % 2 or ix % 2]
    ends.sort(key=lambda p: hops(*p))
    near = [p for p in ends if hops(*p) <= REACH][:tiles]
    owners = [near[t % len(near)] for t in range(tiles)]
    places = [owners[:t].count(owners[t]) for t in range(tiles)]
    return owners, places


def lane_group(rows):
    return iota((rows, LANES), 1) // KY


def pick(parts, group):
    out = parts[0]
    for i, x in list(enumerate(parts))[1:]:
        out = jnp.where(group == i, x, out)
    return out


def expand_cols(parts, col):
    stack = []
    for coef, count, fold in parts:
        group = lane_group(coef.shape[0])
        stack.extend(jnp.where(group == g, coef, 0.0) for g in range(count * fold))
    hi, lo = split(jnp.concatenate(stack, axis=0))
    lhs = jnp.concatenate([hi, lo, hi], axis=1)
    return split(jnp.dot(lhs, col, preferred_element_type=F32))


def expand_rows(hi, lo, row, weight):
    rhs = jnp.concatenate([hi, lo, hi, lo], axis=0)
    return (weight * jnp.dot(row, rhs, preferred_element_type=F32)).astype(BF16)


def analysis_kernel(
    dims, prog_hbm, forc_hbm, strength_hbm, level_hbm, pbl_hbm,
    coef_ref, scale_ref, weight_ref, row_ref, col_ref, early_ref,
    strength, level, pbl, prog, forc, part, mine, got, full, wave,
    load_sem, aux_sem, part_send, part_recv, full_send, full_recv,
):
    gx, gy, tail = dims
    fields, rows, cols = prog.shape
    levels, variables = strength.shape
    n_dev = gx * gy
    groups, tiles = plan_groups(fields)
    owners, places = plan_owners(gx, gy, tiles)
    n_owned = max(places) + 1
    ix, iy = lax.axis_index("gx"), lax.axis_index("gy")
    me = ix * gy + iy
    far = hops(ix, iy)

    def settle(ref, sem):
        pltpu.make_async_copy(ref, ref, sem).wait()

    blocks = plan_blocks(fields)

    def fetch(b):
        span = pl.ds(blocks[b][0], len(blocks[b]))
        odd = len(blocks[b]) % 2
        return (
            pltpu.make_async_copy(prog_hbm.at[span], prog.at[span], load_sem.at[b, 0]),
            pltpu.make_async_copy(forc_hbm.at[span], forc.at[span], load_sem.at[b, odd]),
        )

    def loaded(b):
        count = len(blocks[b])
        if count % 2:
            for copy in fetch(b):
                copy.wait()
        else:
            settle(prog.at[pl.ds(0, count + count // 2)], load_sem.at[b, 0])

    for b in range(len(blocks)):
        for copy in fetch(b):
            copy.start()
    aux = [
        pltpu.make_async_copy(pbl_hbm, pbl, aux_sem.at[0]),
        pltpu.make_async_copy(strength_hbm, strength, aux_sem.at[1]),
        pltpu.make_async_copy(level_hbm, level, aux_sem.at[2]),
    ]
    for copy in aux:
        copy.start()

    def tiles_of(j):
        first, count, fold, tile = groups[j]
        return range(tile, tile + KX // fold // SUB)

    def owned(t):
        return (ix == owners[t][0]) & (iy == owners[t][1])

    def count_owned(k, weigh):
        return sum(
            (owned(t).astype(jnp.int32) * weigh(t) for t in range(tiles) if places[t] == k),
            jnp.int32(0),
        )

    early = len(groups) - tail
    group_of = [min(j, early) for j in range(len(groups)) for t in tiles_of(j)]
    owns = [count_owned(k, lambda t: 1) for k in range(n_owned)]
    tile_at = [count_owned(k, lambda t: t) for k in range(n_owned)]
    group_at = [count_owned(k, lambda t: group_of[t]) for k in range(n_owned)]

    def settle_tiles(buf, sem, first, count, own, most):
        for c in range(min(most, count - 1) + 1):
            pl.when(own == c)(lambda c=c: settle(buf.at[pl.ds(first, count - c)], sem))

    def each_other(act):
        def body(j, carry):
            t = j + (j >= me).astype(jnp.int32)
            act((t // gy, lax.rem(t, gy)))
            return carry
        if n_dev <= 64:
            for j in range(n_dev - 1):
                body(j, 0)
        else:
            lax.fori_loop(0, n_dev - 1, body, 0)

    barrier = pltpu.get_barrier_semaphore()

    @pl.when(owns[0] > 0)
    def _():
        each_other(lambda t: pl.semaphore_signal(barrier, inc=1, device_id=t, device_id_type=MESH))

    def enter():
        pl.semaphore_wait(barrier, len(set(owners)) - owns[0])

    row = basis(
        rows * gx,
        (ix * rows + iota((KX, rows), 1)).astype(F32),
        iota((KX, rows), 0).astype(F32),
    )
    row_hi, row_lo = split(row)
    row_lhs = jnp.concatenate([row_hi, row_lo], axis=0)
    row_lhs = jnp.concatenate([row_lhs, row_lhs], axis=1)
    col = basis(
        cols * gy,
        (iy * cols + iota((cols, LANES), 0)).astype(F32),
        lax.rem(iota((cols, LANES), 1), KY).astype(F32),
    )
    col_rhs = jnp.concatenate(split(col), axis=1)

    def to_owner(t):
        ox, oy = owners[t]
        at = ox * gy + oy
        return pltpu.make_async_remote_copy(
            src_ref=mine.at[t], dst_ref=got.at[places[t], me - (me > at).astype(jnp.int32)],
            send_sem=part_send, recv_sem=part_recv.at[places[t]],
            device_id=(ox, oy), device_id_type=MESH,
        )

    def elsewhere(t, act):
        pl.when(jnp.logical_not(owned(t)))(act)

    def to_all(tile, group, target):
        return pltpu.make_async_remote_copy(
            src_ref=full.at[tile], dst_ref=full.at[tile],
            send_sem=full_send, recv_sem=full_recv.at[group],
            device_id=target, device_id_type=MESH,
        )

    def along_rows(b):
        loaded(b)
        for f in blocks[b]:
            rhs = jnp.concatenate(split(forc[f].astype(F32) - prog[f]), axis=0)
            both = jnp.dot(row_lhs, rhs, preferred_element_type=F32)
            part[f] = both[:KX] + both[KX:]

    def along_cols(j):
        first, count, fold, tile = groups[j]
        hi, lo = split(part[first:first + count].reshape(count * KX, cols))
        both = jnp.dot(hi, col_rhs, preferred_element_type=F32) + jnp.dot(
            lo, col_rhs, preferred_element_type=F32
        )
        both = both[:, :LANES] + both[:, LANES:]
        size = KX // fold
        coef = pick(
            [both[r * size:(r + 1) * size] for r in range(count * fold)], lane_group(size)
        )
        for k, t in enumerate(tiles_of(j)):
            mine[t] = coef[k * SUB:(k + 1) * SUB]

    last = len(groups) - 1
    gate = jnp.where(far >= FAR, 0, jnp.where(far > 0, max(last - 1, 0), last))

    def send(j):
        @pl.when(gate == j)
        def _():
            enter()
            for t in range(tiles_of(j)[0]):
                elsewhere(t, to_owner(t).start)

        @pl.when(gate <= j)
        def _():
            for t in tiles_of(j):
                elsewhere(t, to_owner(t).start)

    ready = 0
    for b in range(len(blocks)):
        along_rows(b)
        if ready < last and blocks[b][0] >= sum(groups[ready][:2]):
            along_cols(ready)
            send(ready)
            ready += 1
    along_cols(last)
    send(last)

    for copy in aux:
        copy.wait()
    for l in range(levels):
        weight_ref[l] = 1.0 / (1.0 + jnp.exp(-(level[l] - pbl[...]) / RAMP_DEPTH))
    for j, (first, count, fold, tile) in enumerate(groups):
        scale = pick(
            [
                jnp.full((SUB, LANES), strength[f // variables, f % variables], F32)
                for f in range(first, first + count)
            ],
            lane_group(SUB) // fold,
        )
        for t in tiles_of(j):
            scale_ref[t * SUB:(t + 1) * SUB] = scale
    col_hi, col_lo = split(basis(
        cols * gy,
        (iy * cols + iota((LANES, cols), 1)).astype(F32),
        lax.rem(iota((LANES, cols), 0), KY).astype(F32),
    ))
    col_ref[...] = jnp.concatenate([col_hi, col_hi, col_lo], axis=0)
    row_hi, row_lo = split(basis(
        rows * gx,
        (ix * rows + iota((rows, 4 * KX), 0)).astype(F32),
        lax.rem(iota((rows, 4 * KX), 1), KX).astype(F32),
    ))
    row_ref[...] = jnp.where(
        iota((rows, 4 * KX), 1) < 2 * KX, row_hi.astype(F32), row_lo.astype(F32)
    ).astype(BF16)

    for k in range(n_owned):
        @pl.when(owns[k] > 0)
        def _(k=k):
            t = tile_at[k]
            settle(got.at[k], part_recv.at[k])
            full[t] = mine[t] + jnp.sum(got[k], axis=0)
            each_other(lambda target: to_all(t, group_at[k], target).start())

    def widen(j):
        first, count, fold, tile = groups[j]
        span = slice(tile * SUB, tile * SUB + KX // fold)
        hi, lo = expand_cols([(coef_ref[span] * scale_ref[span], count, fold)], col_ref[...])
        wave[j % 2, 0, :count * KX] = hi
        wave[j % 2, 1, :count * KX] = lo

    def finish(j):
        first, count, fold, tile = groups[j]
        for k in range(count):
            f = first + k
            span = slice(k * KX, (k + 1) * KX)
            early_ref[f] = expand_rows(
                wave[j % 2, 0, span], wave[j % 2, 1, span], row_ref[...],
                weight_ref[f // variables],
            )

    def arrive(stage):
        here = [t for t in range(tiles) if group_of[t] == stage]
        held = [owners[t] for t in here]
        own = sum((owned(t).astype(jnp.int32) for t in here), jnp.int32(0))
        settle_tiles(
            full, full_recv.at[stage], here[0], len(here), own, max(held.count(o) for o in held)
        )
        for t in here:
            coef_ref[t * SUB:(t + 1) * SUB] = full[t]

    for j in range(early):
        arrive(j)
        widen(j)
        if j:
            finish(j - 1)
    if early:
        finish(early - 1)
    arrive(early)
    settle_tiles(mine, part_send, 0, tiles, sum(owns), n_owned)
    for c in range(1, n_owned + 1):
        pl.when(sum(owns) == c)(lambda c=c: settle(got.at[pl.ds(0, c)], full_send))


def synthesis_kernel(
    tail, coef_ref, scale_ref, weight_ref, row_ref, col_ref, early_ref, tend_hbm, energy_hbm,
    tend, energy_ref, tend_sem, energy_sem,
):
    levels, variables = energy_ref.shape
    fields = levels * variables
    groups, tiles = plan_groups(fields)
    done = groups[-tail][0]

    def out(first, count):
        level, at = first // variables, first % variables
        span = pl.ds(first - done, count) if first >= done else pl.ds(first, count)
        return pltpu.make_async_copy(
            (tend if first >= done else early_ref).at[span],
            tend_hbm.at[level, pl.ds(at, count)],
            tend_sem,
        )

    for first in range(0, done, variables):
        out(first, min(variables, done - first)).start()

    at_row = iota((levels, variables), 0)
    at_col = iota((levels, variables), 1)
    energy = jnp.zeros((levels, variables), F32)
    for first, count, fold, tile in groups:
        coef = coef_ref[tile * SUB:tile * SUB + KX // fold]
        power = jnp.sum(coef * coef, axis=0, keepdims=True)
        group = lane_group(1) // fold
        for k in range(count):
            f = first + k
            one = jnp.sum(jnp.where(group == k, power, 0.0), axis=(0, 1), keepdims=True)
            energy = jnp.where(
                (at_row == f // variables) & (at_col == f % variables), one, energy
            )
    energy_ref[...] = energy * (1.0 / (KX * KY))
    result = pltpu.make_async_copy(energy_ref, energy_hbm, energy_sem)
    result.start()

    parts = []
    for first, count, fold, tile in groups[-tail:]:
        span = slice(tile * SUB, tile * SUB + KX // fold)
        parts.append((coef_ref[span] * scale_ref[span], count, fold))
    hi, lo = expand_cols(parts, col_ref[...])
    for f in range(done, fields):
        span = slice((f - done) * KX, (f - done + 1) * KX)
        tend[f - done] = expand_rows(
            hi[span], lo[span], row_ref[...], weight_ref[f // variables]
        )
        if f > done:
            out(f - 1, 1).start()
    out(fields - 1, 1).start()

    pltpu.make_async_copy(tend_hbm, tend_hbm, tend_sem).wait()
    result.wait()


def per_device(gx, gy, prognostic_values, forcing_host_values, strength, level_height, pbl_height):
    levels, variables, rows, cols = prognostic_values.shape
    fields = levels * variables
    n_dev = gx * gy
    groups, tiles = plan_groups(fields)
    n_owned = max(plan_owners(gx, gy, tiles)[1]) + 1
    tail = min(TAIL, len(groups))
    blocks = plan_blocks(fields)
    done = groups[-tail][0]
    anywhere = pl.BlockSpec(memory_space=pl.ANY)
    vmem = pl.BlockSpec(memory_space=pltpu.VMEM)
    dma = pltpu.SemaphoreType.DMA
    held = pl.pallas_call(
        functools.partial(analysis_kernel, (gx, gy, tail)),
        out_shape=(
            pltpu.VMEM((tiles * SUB, LANES), F32),
            pltpu.VMEM((tiles * SUB, LANES), F32),
            pltpu.VMEM((levels, rows, cols), F32),
            pltpu.VMEM((rows, 4 * KX), BF16),
            pltpu.VMEM((3 * LANES, cols), BF16),
            pltpu.VMEM((max(done, 1), rows, cols), BF16),
        ),
        in_specs=[anywhere] * 5,
        out_specs=(vmem,) * 6,
        scratch_shapes=[
            pltpu.SMEM((levels, variables), F32),
            pltpu.SMEM((levels,), F32),
            pltpu.VMEM((rows, cols), F32),
            pltpu.VMEM((fields, rows, cols), F32),
            pltpu.VMEM((fields, rows, cols), BF16),
            pltpu.VMEM((fields, KX, cols), F32),
            pltpu.VMEM((tiles, SUB, LANES), F32),
            pltpu.VMEM((n_owned, n_dev - 1, SUB, LANES), F32),
            pltpu.VMEM((tiles, SUB, LANES), F32),
            pltpu.VMEM((2, 2, LANES, cols), BF16),
            dma((len(blocks), 1 + max(len(b) % 2 for b in blocks))),
            dma((3,)),
            dma,
            dma((n_owned,)),
            dma,
            dma((len(groups) - tail + 1,)),
        ],
        compiler_params=pltpu.CompilerParams(collective_id=0, has_side_effects=True),
        name="analysis",
    )(
        prognostic_values.reshape(fields, rows, cols),
        forcing_host_values.reshape(fields, rows, cols),
        strength,
        level_height,
        pbl_height,
    )
    tendency, energy = pl.pallas_call(
        functools.partial(synthesis_kernel, tail),
        out_shape=(
            jax.ShapeDtypeStruct((levels, variables, rows, cols), BF16),
            jax.ShapeDtypeStruct((levels, variables), F32),
        ),
        in_specs=[vmem] * 6,
        out_specs=(anywhere, anywhere),
        scratch_shapes=[
            pltpu.VMEM((fields - done, rows, cols), BF16),
            pltpu.VMEM((levels, variables), F32),
            dma,
            dma,
        ],
        name="synthesis",
    )(*[pltpu.with_memory_space_constraint(x, pltpu.VMEM) for x in held])
    return tendency, energy


def solution(mesh):
    return jax.shard_map(
        functools.partial(per_device, mesh.shape["gx"], mesh.shape["gy"]),
        mesh=mesh,
        in_specs=(P(None, None, "gx", "gy"), P(None, None, "gx", "gy"), P(), P(), P("gx", "gy")),
        out_specs=(P(None, None, "gx", "gy"), P()),
        check_vma=False,
    )
```

```python
import functools
import math

import jax
import jax.numpy as jnp
from jax import lax
from jax.experimental import pallas as pl
from jax.experimental.pallas import tpu as pltpu
from jax.sharding import PartitionSpec as P

KX = 32
KY = 32
RAMP_DEPTH = 0.25
LANES = 128
SUB = 8
MESH = pl.DeviceIdType.MESH
REACH = 3
FAR = 3
TAIL = 2
BLOCK = 4

F32 = jnp.float32
BF16 = jnp.bfloat16

SINE = [(-1.0) ** k * (math.pi / 2) ** (2 * k + 1) / math.factorial(2 * k + 1) for k in range(7)]


def basis(total, place, wave):
    turns = (2.0 * place + 1.0) * wave
    rest = turns - (4.0 * total) * jnp.floor(turns * (1.0 / (4.0 * total)))
    t = (jnp.abs(rest - 2.0 * total) - total) * (1.0 / total)
    t2 = t * t
    poly = jnp.full(t.shape, SINE[-1], F32)
    for c in SINE[-2::-1]:
        poly = poly * t2 + c
    scale = jnp.where(wave == 0.0, math.sqrt(1.0 / total), math.sqrt(2.0 / total))
    return scale * (poly * t)


def iota(shape, dim):
    return lax.broadcasted_iota(jnp.int32, shape, dim)


def split(x):
    hi = x.astype(BF16)
    return hi, (x - hi.astype(F32)).astype(BF16)


def hops(ix, iy):
    return ix // 4 + (ix // 2) % 2 + iy


def plan_groups(fields):
    lanes = LANES // KY
    groups = []
    tile = 0
    for first in range(0, fields, lanes):
        count = min(lanes, fields - first)
        fold = lanes // count
        groups.append((first, count, fold, tile))
        tile += KX // fold // SUB
    return groups, tile


def plan_blocks(fields):
    return [range(f, min(f + BLOCK, fields)) for f in range(0, fields, BLOCK)]


def plan_owners(gx, gy, tiles):
    ends = [(ix, iy) for ix in range(gx) for iy in range(gy) if gx % 2 or ix % 2]
    ends.sort(key=lambda p: hops(*p))
    near = [p for p in ends if hops(*p) <= REACH][:tiles]
    owners = [near[t % len(near)] for t in range(tiles)]
    places = [owners[:t].count(owners[t]) for t in range(tiles)]
    return owners, places


def lane_group(rows):
    return iota((rows, LANES), 1) // KY


def pick(parts, group):
    out = parts[0]
    for i, x in list(enumerate(parts))[1:]:
        out = jnp.where(group == i, x, out)
    return out


def expand_cols(parts, col):
    stack = []
    for coef, count, fold in parts:
        group = lane_group(coef.shape[0])
        stack.extend(jnp.where(group == g, coef, 0.0) for g in range(count * fold))
    hi, lo = split(jnp.concatenate(stack, axis=0))
    lhs = jnp.concatenate([hi, lo, hi], axis=1)
    return split(jnp.dot(lhs, col, preferred_element_type=F32))


def expand_rows(hi, lo, row, weight):
    rhs = jnp.concatenate([hi, lo, hi, lo], axis=0)
    return (weight * jnp.dot(row, rhs, preferred_element_type=F32)).astype(BF16)


def analysis_kernel(
    dims, prog_hbm, forc_hbm, strength_hbm, level_hbm, pbl_hbm,
    coef_ref, scale_ref, weight_ref, row_ref, col_ref, early_ref, wide_ref,
    strength, level, pbl, prog, forc, part, mine, got, full, wave,
    load_sem, part_send, part_recv, full_send, full_recv,
):
    gx, gy, tail = dims
    fields, rows, cols = prog.shape
    levels, variables = strength.shape
    n_dev = gx * gy
    groups, tiles = plan_groups(fields)
    owners, places = plan_owners(gx, gy, tiles)
    n_owned = max(places) + 1
    ix, iy = lax.axis_index("gx"), lax.axis_index("gy")
    me = ix * gy + iy
    far = hops(ix, iy)

    def settle(ref, sem):
        pltpu.make_async_copy(ref, ref, sem).wait()

    blocks = plan_blocks(fields)

    def fetch(b):
        span = pl.ds(blocks[b][0], len(blocks[b]))
        odd = len(blocks[b]) % 2
        return (
            pltpu.make_async_copy(prog_hbm.at[span], prog.at[span], load_sem.at[b, 0]),
            pltpu.make_async_copy(forc_hbm.at[span], forc.at[span], load_sem.at[b, odd]),
        )

    def loaded(b):
        count = len(blocks[b])
        if count % 2:
            for copy in fetch(b):
                copy.wait()
        else:
            settle(prog.at[pl.ds(0, count + count // 2)], load_sem.at[b, 0])

    for b in range(len(blocks)):
        for copy in fetch(b):
            copy.start()
    aux = [
        pltpu.make_async_copy(source, target, load_sem.at[i, 0])
        for i, (source, target) in enumerate(
            [(pbl_hbm, pbl), (strength_hbm, strength), (level_hbm, level)]
        )
    ]
    for copy in aux[len(blocks):]:
        copy.start()

    def tiles_of(j):
        first, count, fold, tile = groups[j]
        return range(tile, tile + KX // fold // SUB)

    def owned(t):
        return (ix == owners[t][0]) & (iy == owners[t][1])

    def count_owned(k, weigh):
        return sum(
            (owned(t).astype(jnp.int32) * weigh(t) for t in range(tiles) if places[t] == k),
            jnp.int32(0),
        )

    early = len(groups) - tail
    group_of = [min(j, early) for j in range(len(groups)) for t in tiles_of(j)]
    owns = [count_owned(k, lambda t: 1) for k in range(n_owned)]
    tile_at = [count_owned(k, lambda t: t) for k in range(n_owned)]
    group_at = [count_owned(k, lambda t: group_of[t]) for k in range(n_owned)]

    def settle_tiles(buf, sem, first, count, own, most):
        for c in range(min(most, count - 1) + 1):
            pl.when(own == c)(lambda c=c: settle(buf.at[pl.ds(first, count - c)], sem))

    def each_other(act):
        def body(j, carry):
            t = j + (j >= me).astype(jnp.int32)
            act((t // gy, lax.rem(t, gy)))
            return carry
        if n_dev <= 64:
            for j in range(n_dev - 1):
                body(j, 0)
        else:
            lax.fori_loop(0, n_dev - 1, body, 0)

    barrier = pltpu.get_barrier_semaphore()

    @pl.when(owns[0] > 0)
    def _():
        each_other(lambda t: pl.semaphore_signal(barrier, inc=1, device_id=t, device_id_type=MESH))

    def enter():
        pl.semaphore_wait(barrier, len(set(owners)) - owns[0])

    row = basis(
        rows * gx,
        (ix * rows + iota((KX, rows), 1)).astype(F32),
        iota((KX, rows), 0).astype(F32),
    )
    row_hi, row_lo = split(row)
    row_lhs = jnp.concatenate([row_hi, row_lo], axis=0)
    row_lhs = jnp.concatenate([row_lhs, row_lhs], axis=1)
    col = basis(
        cols * gy,
        (iy * cols + iota((cols, LANES), 0)).astype(F32),
        lax.rem(iota((cols, LANES), 1), KY).astype(F32),
    )
    col_rhs = jnp.concatenate(split(col), axis=1)

    def to_owner(t):
        ox, oy = owners[t]
        at = ox * gy + oy
        return pltpu.make_async_remote_copy(
            src_ref=mine.at[t], dst_ref=got.at[places[t], me - (me > at).astype(jnp.int32)],
            send_sem=part_send, recv_sem=part_recv.at[places[t]],
            device_id=(ox, oy), device_id_type=MESH,
        )

    def elsewhere(t, act):
        pl.when(jnp.logical_not(owned(t)))(act)

    def to_all(tile, group, target):
        return pltpu.make_async_remote_copy(
            src_ref=full.at[tile], dst_ref=full.at[tile],
            send_sem=full_send, recv_sem=full_recv.at[group],
            device_id=target, device_id_type=MESH,
        )

    def along_rows(b):
        loaded(b)
        for f in blocks[b]:
            rhs = jnp.concatenate(split(forc[f].astype(F32) - prog[f]), axis=0)
            both = jnp.dot(row_lhs, rhs, preferred_element_type=F32)
            part[f] = both[:KX] + both[KX:]

    def along_cols(j):
        first, count, fold, tile = groups[j]
        hi, lo = split(part[first:first + count].reshape(count * KX, cols))
        both = jnp.dot(hi, col_rhs, preferred_element_type=F32) + jnp.dot(
            lo, col_rhs, preferred_element_type=F32
        )
        both = both[:, :LANES] + both[:, LANES:]
        size = KX // fold
        coef = pick(
            [both[r * size:(r + 1) * size] for r in range(count * fold)], lane_group(size)
        )
        for k, t in enumerate(tiles_of(j)):
            mine[t] = coef[k * SUB:(k + 1) * SUB]

    last = len(groups) - 1
    gate = jnp.where(far >= FAR, 0, jnp.where(far > 0, max(last - 1, 0), last))

    def send(j):
        @pl.when(gate == j)
        def _():
            enter()
            for t in range(tiles_of(j)[0]):
                elsewhere(t, to_owner(t).start)

        @pl.when(gate <= j)
        def _():
            for t in tiles_of(j):
                elsewhere(t, to_owner(t).start)

    ready = 0
    for b in range(len(blocks)):
        along_rows(b)
        if b < len(aux):
            aux[b].start()
        if ready < last and blocks[b][0] >= sum(groups[ready][:2]):
            along_cols(ready)
            send(ready)
            ready += 1
    along_cols(last)
    send(last)

    for copy in aux:
        copy.wait()
    for l in range(levels):
        weight_ref[l] = 1.0 / (1.0 + jnp.exp(-(level[l] - pbl[...]) / RAMP_DEPTH))
    for j, (first, count, fold, tile) in enumerate(groups):
        scale = pick(
            [
                jnp.full((SUB, LANES), strength[f // variables, f % variables], F32)
                for f in range(first, first + count)
            ],
            lane_group(SUB) // fold,
        )
        for t in tiles_of(j):
            scale_ref[t * SUB:(t + 1) * SUB] = scale
    col_hi, col_lo = split(basis(
        cols * gy,
        (iy * cols + iota((LANES, cols), 1)).astype(F32),
        lax.rem(iota((LANES, cols), 0), KY).astype(F32),
    ))
    col_ref[...] = jnp.concatenate([col_hi, col_hi, col_lo], axis=0)
    row_hi, row_lo = split(basis(
        rows * gx,
        (ix * rows + iota((rows, 4 * KX), 0)).astype(F32),
        lax.rem(iota((rows, 4 * KX), 1), KX).astype(F32),
    ))
    row_ref[...] = jnp.where(
        iota((rows, 4 * KX), 1) < 2 * KX, row_hi.astype(F32), row_lo.astype(F32)
    ).astype(BF16)

    for k in range(n_owned):
        @pl.when(owns[k] > 0)
        def _(k=k):
            t = tile_at[k]
            settle(got.at[k], part_recv.at[k])
            full[t] = mine[t] + jnp.sum(got[k], axis=0)
            each_other(lambda target: to_all(t, group_at[k], target).start())

    def widen(j):
        first, count, fold, tile = groups[j]
        span = slice(tile * SUB, tile * SUB + KX // fold)
        hi, lo = expand_cols([(coef_ref[span] * scale_ref[span], count, fold)], col_ref[...])
        keep = wide_ref if j == early - 1 else wave.at[j % 2]
        keep[0, :count * KX] = hi
        keep[1, :count * KX] = lo

    def finish(j):
        first, count, fold, tile = groups[j]
        for k in range(count):
            f = first + k
            span = slice(k * KX, (k + 1) * KX)
            early_ref[f] = expand_rows(
                wave[j % 2, 0, span], wave[j % 2, 1, span], row_ref[...],
                weight_ref[f // variables],
            )

    def arrive(stage):
        here = [t for t in range(tiles) if group_of[t] == stage]
        held = [owners[t] for t in here]
        own = sum((owned(t).astype(jnp.int32) for t in here), jnp.int32(0))
        settle_tiles(
            full, full_recv.at[stage], here[0], len(here), own, max(held.count(o) for o in held)
        )
        for t in here:
            coef_ref[t * SUB:(t + 1) * SUB] = full[t]

    for j in range(early):
        arrive(j)
        widen(j)
        if j:
            finish(j - 1)
    arrive(early)
    settle_tiles(mine, part_send, 0, tiles, sum(owns), n_owned)
    for c in range(1, n_owned + 1):
        pl.when(sum(owns) == c)(lambda c=c: settle(got.at[pl.ds(0, c)], full_send))


def synthesis_kernel(
    tail, coef_ref, scale_ref, weight_ref, row_ref, col_ref, early_ref, wide_ref,
    tend_hbm, energy_hbm,
    tend, energy_ref, tend_sem, energy_sem,
):
    levels, variables = energy_ref.shape
    fields = levels * variables
    groups, tiles = plan_groups(fields)
    done, wide = groups[-tail - 1][:2]

    def out(first, count):
        level, at = first // variables, first % variables
        span = pl.ds(first - done, count) if first >= done else pl.ds(first, count)
        return pltpu.make_async_copy(
            (tend if first >= done else early_ref).at[span],
            tend_hbm.at[level, pl.ds(at, count)],
            tend_sem,
        )

    for first in range(0, done, variables):
        out(first, min(variables, done - first)).start()

    at_row = iota((levels, variables), 0)
    at_col = iota((levels, variables), 1)
    energy = jnp.zeros((levels, variables), F32)
    for first, count, fold, tile in groups:
        coef = coef_ref[tile * SUB:tile * SUB + KX // fold]
        power = jnp.sum(coef * coef, axis=0, keepdims=True)
        group = lane_group(1) // fold
        for k in range(count):
            f = first + k
            one = jnp.sum(jnp.where(group == k, power, 0.0), axis=(0, 1), keepdims=True)
            energy = jnp.where(
                (at_row == f // variables) & (at_col == f % variables), one, energy
            )
    energy_ref[...] = energy * (1.0 / (KX * KY))
    result = pltpu.make_async_copy(energy_ref, energy_hbm, energy_sem)
    result.start()

    parts = []
    for first, count, fold, tile in groups[-tail:]:
        span = slice(tile * SUB, tile * SUB + KX // fold)
        parts.append((coef_ref[span] * scale_ref[span], count, fold))
    hi, lo = expand_cols(parts, col_ref[...])
    for f in range(done, fields):
        k = f - done if f < done + wide else f - done - wide
        span = slice(k * KX, (k + 1) * KX)
        pair = (wide_ref[0, span], wide_ref[1, span]) if f < done + wide else (hi[span], lo[span])
        tend[f - done] = expand_rows(*pair, row_ref[...], weight_ref[f // variables])
        if f > done:
            out(f - 1, 1).start()
    out(fields - 1, 1).start()

    pltpu.make_async_copy(tend_hbm, tend_hbm, tend_sem).wait()
    result.wait()


def per_device(gx, gy, prognostic_values, forcing_host_values, strength, level_height, pbl_height):
    levels, variables, rows, cols = prognostic_values.shape
    fields = levels * variables
    n_dev = gx * gy
    groups, tiles = plan_groups(fields)
    n_owned = max(plan_owners(gx, gy, tiles)[1]) + 1
    tail = min(TAIL, len(groups) - 1)
    blocks = plan_blocks(fields)
    done = groups[-tail - 1][0]
    anywhere = pl.BlockSpec(memory_space=pl.ANY)
    vmem = pl.BlockSpec(memory_space=pltpu.VMEM)
    dma = pltpu.SemaphoreType.DMA
    held = pl.pallas_call(
        functools.partial(analysis_kernel, (gx, gy, tail)),
        out_shape=(
            pltpu.VMEM((tiles * SUB, LANES), F32),
            pltpu.VMEM((tiles * SUB, LANES), F32),
            pltpu.VMEM((levels, rows, cols), F32),
            pltpu.VMEM((rows, 4 * KX), BF16),
            pltpu.VMEM((3 * LANES, cols), BF16),
            pltpu.VMEM((max(done, 1), rows, cols), BF16),
            pltpu.VMEM((2, LANES, cols), BF16),
        ),
        in_specs=[anywhere] * 5,
        out_specs=(vmem,) * 7,
        scratch_shapes=[
            pltpu.SMEM((levels, variables), F32),
            pltpu.SMEM((levels,), F32),
            pltpu.VMEM((rows, cols), F32),
            pltpu.VMEM((fields, rows, cols), F32),
            pltpu.VMEM((fields, rows, cols), BF16),
            pltpu.VMEM((fields, KX, cols), F32),
            pltpu.VMEM((tiles, SUB, LANES), F32),
            pltpu.VMEM((n_owned, n_dev - 1, SUB, LANES), F32),
            pltpu.VMEM((tiles, SUB, LANES), F32),
            pltpu.VMEM((2, 2, LANES, cols), BF16),
            dma((max(len(blocks), 3), 1 + max(len(b) % 2 for b in blocks))),
            dma,
            dma((n_owned,)),
            dma,
            dma((len(groups) - tail + 1,)),
        ],
        compiler_params=pltpu.CompilerParams(collective_id=0, has_side_effects=True),
        name="analysis",
    )(
        prognostic_values.reshape(fields, rows, cols),
        forcing_host_values.reshape(fields, rows, cols),
        strength,
        level_height,
        pbl_height,
    )
    tendency, energy = pl.pallas_call(
        functools.partial(synthesis_kernel, tail),
        out_shape=(
            jax.ShapeDtypeStruct((levels, variables, rows, cols), BF16),
            jax.ShapeDtypeStruct((levels, variables), F32),
        ),
        in_specs=[vmem] * 7,
        out_specs=(anywhere, anywhere),
        scratch_shapes=[
            pltpu.VMEM((fields - done, rows, cols), BF16),
            pltpu.VMEM((levels, variables), F32),
            dma,
            dma,
        ],
        name="synthesis",
    )(*[pltpu.with_memory_space_constraint(x, pltpu.VMEM) for x in held])
    return tendency, energy


def solution(mesh):
    return jax.shard_map(
        functools.partial(per_device, mesh.shape["gx"], mesh.shape["gy"]),
        mesh=mesh,
        in_specs=(P(None, None, "gx", "gy"), P(None, None, "gx", "gy"), P(), P(), P("gx", "gy")),
        out_specs=(P(None, None, "gx", "gy"), P()),
        check_vma=False,
    )
```

```python
import functools
import math

import jax
import jax.numpy as jnp
from jax import lax
from jax.experimental import pallas as pl
from jax.experimental.pallas import tpu as pltpu
from jax.sharding import PartitionSpec as P

KX = 32
KY = 32
RAMP_DEPTH = 0.25
LANES = 128
SUB = 8
MESH = pl.DeviceIdType.MESH
REACH = 3
EARLY = 4
TAIL = 2
BLOCK = 4

F32 = jnp.float32
BF16 = jnp.bfloat16

SINE = [(-1.0) ** k * (math.pi / 2) ** (2 * k + 1) / math.factorial(2 * k + 1) for k in range(7)]


def basis(total, place, wave):
    turns = (2.0 * place + 1.0) * wave
    rest = turns - (4.0 * total) * jnp.floor(turns * (1.0 / (4.0 * total)))
    t = (jnp.abs(rest - 2.0 * total) - total) * (1.0 / total)
    t2 = t * t
    poly = jnp.full(t.shape, SINE[-1], F32)
    for c in SINE[-2::-1]:
        poly = poly * t2 + c
    scale = jnp.where(wave == 0.0, math.sqrt(1.0 / total), math.sqrt(2.0 / total))
    return scale * (poly * t)


def iota(shape, dim):
    return lax.broadcasted_iota(jnp.int32, shape, dim)


def split(x):
    hi = x.astype(BF16)
    return hi, (x - hi.astype(F32)).astype(BF16)


def hops(ix, iy):
    return ix // 4 + (ix // 2) % 2 + iy


def plan_groups(fields):
    lanes = LANES // KY
    groups = []
    tile = 0
    for first in range(0, fields, lanes):
        count = min(lanes, fields - first)
        fold = lanes // count
        groups.append((first, count, fold, tile))
        tile += KX // fold // SUB
    return groups, tile


def plan_blocks(fields):
    return [range(f, min(f + BLOCK, fields)) for f in range(0, fields, BLOCK)]


def plan_owners(gx, gy, tiles):
    ends = [(ix, iy) for ix in range(gx) for iy in range(gy) if gx % 2 or ix % 2]
    ends.sort(key=lambda p: hops(*p))
    near = [p for p in ends if hops(*p) <= REACH][:tiles]
    owners = [near[t % len(near)] for t in range(tiles)]
    places = [owners[:t].count(owners[t]) for t in range(tiles)]
    return owners, places


def plan_gates(gx, gy, owners, last):
    def spot(p):
        return p[0] // 4, (p[0] // 2) % 2, p[1]

    def wait(p):
        apart = [sum(abs(a - b) for a, b in zip(spot(p), spot(o))) for o in owners]
        return max(hops(*o) + d for o, d in zip(owners, apart)) - hops(*p)

    every = [(ix, iy) for ix in range(gx) for iy in range(gy)]
    return [
        (p, min(max(wait(p) - EARLY, 0), last) if hops(*p) else last) for p in every
    ]


def lane_group(rows):
    return iota((rows, LANES), 1) // KY


def pick(parts, group):
    out = parts[0]
    for i, x in list(enumerate(parts))[1:]:
        out = jnp.where(group == i, x, out)
    return out


def expand_cols(parts, col):
    stack = []
    for coef, count, fold in parts:
        group = lane_group(coef.shape[0])
        stack.extend(jnp.where(group == g, coef, 0.0) for g in range(count * fold))
    hi, lo = split(jnp.concatenate(stack, axis=0))
    lhs = jnp.concatenate([hi, lo, hi], axis=1)
    return split(jnp.dot(lhs, col, preferred_element_type=F32))


def expand_rows(hi, lo, row, weight):
    rhs = jnp.concatenate([hi, lo, hi, lo], axis=0)
    return (weight * jnp.dot(row, rhs, preferred_element_type=F32)).astype(BF16)


def analysis_kernel(
    dims, prog_hbm, forc_hbm, strength_hbm, level_hbm, pbl_hbm,
    coef_ref, scale_ref, weight_ref, row_ref, col_ref, early_ref, wide_ref,
    strength, level, pbl, prog, forc, part, mine, got, full, wave,
    load_sem, part_send, part_recv, full_send, full_recv,
):
    gx, gy, tail = dims
    fields, rows, cols = prog.shape
    levels, variables = strength.shape
    n_dev = gx * gy
    groups, tiles = plan_groups(fields)
    owners, places = plan_owners(gx, gy, tiles)
    n_owned = max(places) + 1
    ix, iy = lax.axis_index("gx"), lax.axis_index("gy")
    me = ix * gy + iy

    def at(p):
        return (ix == p[0]) & (iy == p[1])


    def settle(ref, sem):
        pltpu.make_async_copy(ref, ref, sem).wait()

    blocks = plan_blocks(fields)

    def fetch(b):
        span = pl.ds(blocks[b][0], len(blocks[b]))
        odd = len(blocks[b]) % 2
        return (
            pltpu.make_async_copy(prog_hbm.at[span], prog.at[span], load_sem.at[b, 0]),
            pltpu.make_async_copy(forc_hbm.at[span], forc.at[span], load_sem.at[b, odd]),
        )

    def loaded(b):
        count = len(blocks[b])
        if count % 2:
            for copy in fetch(b):
                copy.wait()
        else:
            settle(prog.at[pl.ds(0, count + count // 2)], load_sem.at[b, 0])

    for b in range(len(blocks)):
        for copy in fetch(b):
            copy.start()
    aux = [
        pltpu.make_async_copy(source, target, load_sem.at[i, 0])
        for i, (source, target) in enumerate(
            [(pbl_hbm, pbl), (strength_hbm, strength), (level_hbm, level)]
        )
    ]
    for copy in aux[len(blocks):]:
        copy.start()

    def tiles_of(j):
        first, count, fold, tile = groups[j]
        return range(tile, tile + KX // fold // SUB)

    def owned(t):
        return at(owners[t])

    def count_owned(k, weigh):
        return sum(
            (owned(t).astype(jnp.int32) * weigh(t) for t in range(tiles) if places[t] == k),
            jnp.int32(0),
        )

    early = len(groups) - tail
    group_of = [min(j, early) for j in range(len(groups)) for t in tiles_of(j)]
    owns = [count_owned(k, lambda t: 1) for k in range(n_owned)]
    tile_at = [count_owned(k, lambda t: t) for k in range(n_owned)]
    group_at = [count_owned(k, lambda t: group_of[t]) for k in range(n_owned)]

    def settle_tiles(buf, sem, first, count, own, most):
        for c in range(min(most, count - 1) + 1):
            pl.when(own == c)(lambda c=c: settle(buf.at[pl.ds(first, count - c)], sem))

    def each_other(act):
        def body(j, carry):
            t = j + (j >= me).astype(jnp.int32)
            act((t // gy, lax.rem(t, gy)))
            return carry
        if n_dev <= 64:
            for j in range(n_dev - 1):
                body(j, 0)
        else:
            lax.fori_loop(0, n_dev - 1, body, 0)

    barrier = pltpu.get_barrier_semaphore()

    @pl.when(owns[0] > 0)
    def _():
        each_other(lambda t: pl.semaphore_signal(barrier, inc=1, device_id=t, device_id_type=MESH))

    def enter():
        pl.semaphore_wait(barrier, len(set(owners)) - owns[0])

    row = basis(
        rows * gx,
        (ix * rows + iota((KX, rows), 1)).astype(F32),
        iota((KX, rows), 0).astype(F32),
    )
    row_hi, row_lo = split(row)
    row_lhs = jnp.concatenate([row_hi, row_lo], axis=0)
    row_lhs = jnp.concatenate([row_lhs, row_lhs], axis=1)
    col = basis(
        cols * gy,
        (iy * cols + iota((cols, LANES), 0)).astype(F32),
        lax.rem(iota((cols, LANES), 1), KY).astype(F32),
    )
    col_rhs = jnp.concatenate(split(col), axis=1)

    def to_owner(t):
        ox, oy = owners[t]
        at = ox * gy + oy
        return pltpu.make_async_remote_copy(
            src_ref=mine.at[t], dst_ref=got.at[places[t], me - (me > at).astype(jnp.int32)],
            send_sem=part_send, recv_sem=part_recv.at[places[t]],
            device_id=(ox, oy), device_id_type=MESH,
        )

    def elsewhere(t, act):
        pl.when(jnp.logical_not(owned(t)))(act)

    def to_all(tile, group, target):
        return pltpu.make_async_remote_copy(
            src_ref=full.at[tile], dst_ref=full.at[tile],
            send_sem=full_send, recv_sem=full_recv.at[group],
            device_id=target, device_id_type=MESH,
        )

    def along_rows(b):
        loaded(b)
        for f in blocks[b]:
            rhs = jnp.concatenate(split(forc[f].astype(F32) - prog[f]), axis=0)
            both = jnp.dot(row_lhs, rhs, preferred_element_type=F32)
            part[f] = both[:KX] + both[KX:]

    def along_cols(j):
        first, count, fold, tile = groups[j]
        hi, lo = split(part[first:first + count].reshape(count * KX, cols))
        both = jnp.dot(hi, col_rhs, preferred_element_type=F32) + jnp.dot(
            lo, col_rhs, preferred_element_type=F32
        )
        both = both[:, :LANES] + both[:, LANES:]
        size = KX // fold
        coef = pick(
            [both[r * size:(r + 1) * size] for r in range(count * fold)], lane_group(size)
        )
        for k, t in enumerate(tiles_of(j)):
            mine[t] = coef[k * SUB:(k + 1) * SUB]

    last = len(groups) - 1
    gate = sum(
        (at(p).astype(jnp.int32) * g for p, g in plan_gates(gx, gy, owners, last) if g),
        jnp.int32(0),
    )

    def send(j):
        @pl.when(gate == j)
        def _():
            enter()
            for t in range(tiles_of(j)[0]):
                elsewhere(t, to_owner(t).start)

        @pl.when(gate <= j)
        def _():
            for t in tiles_of(j):
                elsewhere(t, to_owner(t).start)

    ready = 0
    for b in range(len(blocks)):
        along_rows(b)
        if b < len(aux):
            aux[b].start()
        if ready < last and blocks[b][0] >= sum(groups[ready][:2]):
            along_cols(ready)
            send(ready)
            ready += 1
    along_cols(last)
    send(last)

    for copy in aux:
        copy.wait()
    for l in range(levels):
        weight_ref[l] = 1.0 / (1.0 + jnp.exp(-(level[l] - pbl[...]) / RAMP_DEPTH))
    for j, (first, count, fold, tile) in enumerate(groups):
        scale = pick(
            [
                jnp.full((SUB, LANES), strength[f // variables, f % variables], F32)
                for f in range(first, first + count)
            ],
            lane_group(SUB) // fold,
        )
        for t in tiles_of(j):
            scale_ref[t * SUB:(t + 1) * SUB] = scale
    col_hi, col_lo = split(basis(
        cols * gy,
        (iy * cols + iota((LANES, cols), 1)).astype(F32),
        lax.rem(iota((LANES, cols), 0), KY).astype(F32),
    ))
    col_ref[...] = jnp.concatenate([col_hi, col_hi, col_lo], axis=0)
    row_hi, row_lo = split(basis(
        rows * gx,
        (ix * rows + iota((rows, 4 * KX), 0)).astype(F32),
        lax.rem(iota((rows, 4 * KX), 1), KX).astype(F32),
    ))
    row_ref[...] = jnp.where(
        iota((rows, 4 * KX), 1) < 2 * KX, row_hi.astype(F32), row_lo.astype(F32)
    ).astype(BF16)

    for k in range(n_owned):
        @pl.when(owns[k] > 0)
        def _(k=k):
            t = tile_at[k]
            settle(got.at[k], part_recv.at[k])
            full[t] = mine[t] + jnp.sum(got[k], axis=0)
            each_other(lambda target: to_all(t, group_at[k], target).start())

    def widen(j):
        first, count, fold, tile = groups[j]
        span = slice(tile * SUB, tile * SUB + KX // fold)
        hi, lo = expand_cols([(coef_ref[span] * scale_ref[span], count, fold)], col_ref[...])
        keep = wide_ref if j == early - 1 else wave.at[j % 2]
        keep[0, :count * KX] = hi
        keep[1, :count * KX] = lo

    def finish(j):
        first, count, fold, tile = groups[j]
        for k in range(count):
            f = first + k
            span = slice(k * KX, (k + 1) * KX)
            early_ref[f] = expand_rows(
                wave[j % 2, 0, span], wave[j % 2, 1, span], row_ref[...],
                weight_ref[f // variables],
            )

    def arrive(stage):
        here = [t for t in range(tiles) if group_of[t] == stage]
        held = [owners[t] for t in here]
        own = sum((owned(t).astype(jnp.int32) for t in here), jnp.int32(0))
        settle_tiles(
            full, full_recv.at[stage], here[0], len(here), own, max(held.count(o) for o in held)
        )
        for t in here:
            coef_ref[t * SUB:(t + 1) * SUB] = full[t]

    for j in range(early):
        arrive(j)
        widen(j)
        if j:
            finish(j - 1)
    arrive(early)
    settle_tiles(mine, part_send, 0, tiles, sum(owns), n_owned)
    for c in range(1, n_owned + 1):
        pl.when(sum(owns) == c)(lambda c=c: settle(got.at[pl.ds(0, c)], full_send))


def synthesis_kernel(
    tail, coef_ref, scale_ref, weight_ref, row_ref, col_ref, early_ref, wide_ref,
    tend_hbm, energy_hbm,
    tend, energy_ref, tend_sem, energy_sem,
):
    levels, variables = energy_ref.shape
    fields = levels * variables
    groups, tiles = plan_groups(fields)
    done, wide = groups[-tail - 1][:2]

    def out(first, count):
        level, at = first // variables, first % variables
        span = pl.ds(first - done, count) if first >= done else pl.ds(first, count)
        return pltpu.make_async_copy(
            (tend if first >= done else early_ref).at[span],
            tend_hbm.at[level, pl.ds(at, count)],
            tend_sem,
        )

    for first in range(0, done, variables):
        out(first, min(variables, done - first)).start()

    at_row = iota((levels, variables), 0)
    at_col = iota((levels, variables), 1)
    energy = jnp.zeros((levels, variables), F32)
    for first, count, fold, tile in groups:
        coef = coef_ref[tile * SUB:tile * SUB + KX // fold]
        power = jnp.sum(coef * coef, axis=0, keepdims=True)
        group = lane_group(1) // fold
        for k in range(count):
            f = first + k
            one = jnp.sum(jnp.where(group == k, power, 0.0), axis=(0, 1), keepdims=True)
            energy = jnp.where(
                (at_row == f // variables) & (at_col == f % variables), one, energy
            )
    energy_ref[...] = energy * (1.0 / (KX * KY))
    result = pltpu.make_async_copy(energy_ref, energy_hbm, energy_sem)
    result.start()

    parts = []
    for first, count, fold, tile in groups[-tail:]:
        span = slice(tile * SUB, tile * SUB + KX // fold)
        parts.append((coef_ref[span] * scale_ref[span], count, fold))
    hi, lo = expand_cols(parts, col_ref[...])
    for f in range(done, fields):
        k = f - done if f < done + wide else f - done - wide
        span = slice(k * KX, (k + 1) * KX)
        pair = (wide_ref[0, span], wide_ref[1, span]) if f < done + wide else (hi[span], lo[span])
        tend[f - done] = expand_rows(*pair, row_ref[...], weight_ref[f // variables])
        if f > done:
            out(f - 1, 1).start()
    out(fields - 1, 1).start()

    pltpu.make_async_copy(tend_hbm, tend_hbm, tend_sem).wait()
    result.wait()


def per_device(gx, gy, prognostic_values, forcing_host_values, strength, level_height, pbl_height):
    levels, variables, rows, cols = prognostic_values.shape
    fields = levels * variables
    n_dev = gx * gy
    groups, tiles = plan_groups(fields)
    n_owned = max(plan_owners(gx, gy, tiles)[1]) + 1
    tail = min(TAIL, len(groups) - 1)
    blocks = plan_blocks(fields)
    done = groups[-tail - 1][0]
    anywhere = pl.BlockSpec(memory_space=pl.ANY)
    vmem = pl.BlockSpec(memory_space=pltpu.VMEM)
    dma = pltpu.SemaphoreType.DMA
    held = pl.pallas_call(
        functools.partial(analysis_kernel, (gx, gy, tail)),
        out_shape=(
            pltpu.VMEM((tiles * SUB, LANES), F32),
            pltpu.VMEM((tiles * SUB, LANES), F32),
            pltpu.VMEM((levels, rows, cols), F32),
            pltpu.VMEM((rows, 4 * KX), BF16),
            pltpu.VMEM((3 * LANES, cols), BF16),
            pltpu.VMEM((max(done, 1), rows, cols), BF16),
            pltpu.VMEM((2, LANES, cols), BF16),
        ),
        in_specs=[anywhere] * 5,
        out_specs=(vmem,) * 7,
        scratch_shapes=[
            pltpu.SMEM((levels, variables), F32),
            pltpu.SMEM((levels,), F32),
            pltpu.VMEM((rows, cols), F32),
            pltpu.VMEM((fields, rows, cols), F32),
            pltpu.VMEM((fields, rows, cols), BF16),
            pltpu.VMEM((fields, KX, cols), F32),
            pltpu.VMEM((tiles, SUB, LANES), F32),
            pltpu.VMEM((n_owned, n_dev - 1, SUB, LANES), F32),
            pltpu.VMEM((tiles, SUB, LANES), F32),
            pltpu.VMEM((2, 2, LANES, cols), BF16),
            dma((max(len(blocks), 3), 1 + max(len(b) % 2 for b in blocks))),
            dma,
            dma((n_owned,)),
            dma,
            dma((len(groups) - tail + 1,)),
        ],
        compiler_params=pltpu.CompilerParams(collective_id=0, has_side_effects=True),
        name="analysis",
    )(
        prognostic_values.reshape(fields, rows, cols),
        forcing_host_values.reshape(fields, rows, cols),
        strength,
        level_height,
        pbl_height,
    )
    tendency, energy = pl.pallas_call(
        functools.partial(synthesis_kernel, tail),
        out_shape=(
            jax.ShapeDtypeStruct((levels, variables, rows, cols), BF16),
            jax.ShapeDtypeStruct((levels, variables), F32),
        ),
        in_specs=[vmem] * 7,
        out_specs=(anywhere, anywhere),
        scratch_shapes=[
            pltpu.VMEM((fields - done, rows, cols), BF16),
            pltpu.VMEM((levels, variables), F32),
            dma,
            dma,
        ],
        name="synthesis",
    )(*[pltpu.with_memory_space_constraint(x, pltpu.VMEM) for x in held])
    return tendency, energy


def solution(mesh):
    return jax.shard_map(
        functools.partial(per_device, mesh.shape["gx"], mesh.shape["gy"]),
        mesh=mesh,
        in_specs=(P(None, None, "gx", "gy"), P(None, None, "gx", "gy"), P(), P(), P("gx", "gy")),
        out_specs=(P(None, None, "gx", "gy"), P()),
        check_vma=False,
    )
```

```python
import functools
import math

import jax
import jax.numpy as jnp
from jax import lax
from jax.experimental import pallas as pl
from jax.experimental.pallas import tpu as pltpu
from jax.sharding import PartitionSpec as P

KX = 32
KY = 32
RAMP_DEPTH = 0.25
LANES = 128
SUB = 8
MESH = pl.DeviceIdType.MESH
REACH = 3
EARLY = 4
TAIL = 2
BLOCK = 4

F32 = jnp.float32
BF16 = jnp.bfloat16

SINE = [(-1.0) ** k * (math.pi / 2) ** (2 * k + 1) / math.factorial(2 * k + 1) for k in range(7)]


def basis(total, place, wave):
    turns = (2.0 * place + 1.0) * wave
    rest = turns - (4.0 * total) * jnp.floor(turns * (1.0 / (4.0 * total)))
    t = (jnp.abs(rest - 2.0 * total) - total) * (1.0 / total)
    t2 = t * t
    poly = jnp.full(t.shape, SINE[-1], F32)
    for c in SINE[-2::-1]:
        poly = poly * t2 + c
    scale = jnp.where(wave == 0.0, math.sqrt(1.0 / total), math.sqrt(2.0 / total))
    return scale * (poly * t)


def iota(shape, dim):
    return lax.broadcasted_iota(jnp.int32, shape, dim)


def split(x):
    hi = x.astype(BF16)
    return hi, (x - hi.astype(F32)).astype(BF16)


def hops(ix, iy):
    return ix // 4 + (ix // 2) % 2 + iy


def plan_groups(fields):
    lanes = LANES // KY
    groups = []
    tile = 0
    for first in range(0, fields, lanes):
        count = min(lanes, fields - first)
        fold = lanes // count
        groups.append((first, count, fold, tile))
        tile += KX // fold // SUB
    return groups, tile


def plan_blocks(fields):
    return [range(f, min(f + BLOCK, fields)) for f in range(0, fields, BLOCK)]


def plan_owners(gx, gy, tiles):
    ends = [(ix, iy) for ix in range(gx) for iy in range(gy) if gx % 2 or ix % 2]
    ends.sort(key=lambda p: hops(*p))
    near = [p for p in ends if hops(*p) <= REACH][:tiles]
    owners = [near[t % len(near)] for t in range(tiles)]
    places = [owners[:t].count(owners[t]) for t in range(tiles)]
    return owners, places


def plan_gates(gx, gy, owners, last):
    def spot(p):
        return p[0] // 4, (p[0] // 2) % 2, p[1]

    def wait(p):
        apart = [sum(abs(a - b) for a, b in zip(spot(p), spot(o))) for o in owners]
        return max(hops(*o) + d for o, d in zip(owners, apart)) - hops(*p)

    every = [(ix, iy) for ix in range(gx) for iy in range(gy)]
    return [
        (p, min(max(wait(p) - EARLY, 0), last) if hops(*p) else last) for p in every
    ]


def add_tiles(got, k):
    count = got.shape[1]
    if count > 64:
        return jnp.sum(got[k], axis=0)
    terms = [got[k, i] for i in range(count)]
    while len(terms) > 1:
        odd = terms[len(terms) & ~1:]
        terms = [x + y for x, y in zip(terms[::2], terms[1::2])] + odd
    return terms[0]


def lane_group(rows):
    return iota((rows, LANES), 1) // KY


def pick(parts, group):
    out = parts[0]
    for i, x in list(enumerate(parts))[1:]:
        out = jnp.where(group == i, x, out)
    return out


def expand_cols(parts, col):
    stack = []
    for coef, count, fold in parts:
        group = lane_group(coef.shape[0])
        stack.extend(jnp.where(group == g, coef, 0.0) for g in range(count * fold))
    hi, lo = split(jnp.concatenate(stack, axis=0))
    lhs = jnp.concatenate([hi, lo, hi], axis=1)
    return split(jnp.dot(lhs, col, preferred_element_type=F32))


def expand_rows(hi, lo, row, weight):
    rhs = jnp.concatenate([hi, lo, hi, lo], axis=0)
    return (weight * jnp.dot(row, rhs, preferred_element_type=F32)).astype(BF16)


def analysis_kernel(
    dims, prog_hbm, forc_hbm, strength_hbm, level_hbm, pbl_hbm,
    coef_ref, scale_ref, weight_ref, row_ref, col_ref, early_ref, wide_ref,
    strength, level, pbl, prog, forc, part, mine, got, full, wave,
    load_sem, part_send, part_recv, full_send, full_recv,
):
    gx, gy, tail = dims
    fields, rows, cols = prog.shape
    levels, variables = strength.shape
    n_dev = gx * gy
    groups, tiles = plan_groups(fields)
    owners, places = plan_owners(gx, gy, tiles)
    n_owned = max(places) + 1
    ix, iy = lax.axis_index("gx"), lax.axis_index("gy")
    me = ix * gy + iy

    def at(p):
        return (ix == p[0]) & (iy == p[1])


    def settle(ref, sem):
        pltpu.make_async_copy(ref, ref, sem).wait()

    blocks = plan_blocks(fields)

    def fetch(b):
        span = pl.ds(blocks[b][0], len(blocks[b]))
        odd = len(blocks[b]) % 2
        return (
            pltpu.make_async_copy(prog_hbm.at[span], prog.at[span], load_sem.at[b, 0]),
            pltpu.make_async_copy(forc_hbm.at[span], forc.at[span], load_sem.at[b, odd]),
        )

    def loaded(b):
        count = len(blocks[b])
        if count % 2:
            for copy in fetch(b):
                copy.wait()
        else:
            settle(prog.at[pl.ds(0, count + count // 2)], load_sem.at[b, 0])

    for b in range(len(blocks)):
        for copy in fetch(b):
            copy.start()
    aux = [
        pltpu.make_async_copy(source, target, load_sem.at[i, 0])
        for i, (source, target) in enumerate(
            [(pbl_hbm, pbl), (strength_hbm, strength), (level_hbm, level)]
        )
    ]
    for copy in aux[len(blocks):]:
        copy.start()

    def tiles_of(j):
        first, count, fold, tile = groups[j]
        return range(tile, tile + KX // fold // SUB)

    def owned(t):
        return at(owners[t])

    def count_owned(k, weigh):
        return sum(
            (owned(t).astype(jnp.int32) * weigh(t) for t in range(tiles) if places[t] == k),
            jnp.int32(0),
        )

    early = len(groups) - tail
    group_of = [min(j, early) for j in range(len(groups)) for t in tiles_of(j)]
    owns = [count_owned(k, lambda t: 1) for k in range(n_owned)]
    tile_at = [count_owned(k, lambda t: t) for k in range(n_owned)]
    group_at = [count_owned(k, lambda t: group_of[t]) for k in range(n_owned)]

    def settle_tiles(buf, sem, first, count, own, most):
        for c in range(min(most, count - 1) + 1):
            pl.when(own == c)(lambda c=c: settle(buf.at[pl.ds(first, count - c)], sem))

    def each_other(act):
        def body(j, carry):
            t = j + (j >= me).astype(jnp.int32)
            act((t // gy, lax.rem(t, gy)))
            return carry
        if n_dev <= 64:
            for j in range(n_dev - 1):
                body(j, 0)
        else:
            lax.fori_loop(0, n_dev - 1, body, 0)

    barrier = pltpu.get_barrier_semaphore()

    @pl.when(owns[0] > 0)
    def _():
        each_other(lambda t: pl.semaphore_signal(barrier, inc=1, device_id=t, device_id_type=MESH))

    def enter():
        pl.semaphore_wait(barrier, len(set(owners)) - owns[0])

    row = basis(
        rows * gx,
        (ix * rows + iota((KX, rows), 1)).astype(F32),
        iota((KX, rows), 0).astype(F32),
    )
    row_hi, row_lo = split(row)
    row_lhs = jnp.concatenate([row_hi, row_lo], axis=0)
    row_lhs = jnp.concatenate([row_lhs, row_lhs], axis=1)
    col = basis(
        cols * gy,
        (iy * cols + iota((cols, LANES), 0)).astype(F32),
        lax.rem(iota((cols, LANES), 1), KY).astype(F32),
    )
    col_rhs = jnp.concatenate(split(col), axis=1)

    def to_owner(t):
        ox, oy = owners[t]
        at = ox * gy + oy
        return pltpu.make_async_remote_copy(
            src_ref=mine.at[t], dst_ref=got.at[places[t], me - (me > at).astype(jnp.int32)],
            send_sem=part_send, recv_sem=part_recv.at[places[t]],
            device_id=(ox, oy), device_id_type=MESH,
        )

    def elsewhere(t, act):
        pl.when(jnp.logical_not(owned(t)))(act)

    def to_all(tile, group, target):
        return pltpu.make_async_remote_copy(
            src_ref=full.at[tile], dst_ref=full.at[tile],
            send_sem=full_send, recv_sem=full_recv.at[group],
            device_id=target, device_id_type=MESH,
        )

    def along_rows(b):
        loaded(b)
        for f in blocks[b]:
            rhs = jnp.concatenate(split(forc[f].astype(F32) - prog[f]), axis=0)
            both = jnp.dot(row_lhs, rhs, preferred_element_type=F32)
            part[f] = both[:KX] + both[KX:]

    def along_cols(j):
        first, count, fold, tile = groups[j]
        hi, lo = split(part[first:first + count].reshape(count * KX, cols))
        both = jnp.dot(hi, col_rhs, preferred_element_type=F32) + jnp.dot(
            lo, col_rhs, preferred_element_type=F32
        )
        both = both[:, :LANES] + both[:, LANES:]
        size = KX // fold
        coef = pick(
            [both[r * size:(r + 1) * size] for r in range(count * fold)], lane_group(size)
        )
        for k, t in enumerate(tiles_of(j)):
            mine[t] = coef[k * SUB:(k + 1) * SUB]

    last = len(groups) - 1
    gate = sum(
        (at(p).astype(jnp.int32) * g for p, g in plan_gates(gx, gy, owners, last) if g),
        jnp.int32(0),
    )

    def send(j):
        @pl.when(gate == j)
        def _():
            enter()
            for t in range(tiles_of(j)[0]):
                elsewhere(t, to_owner(t).start)

        @pl.when(gate <= j)
        def _():
            for t in tiles_of(j):
                elsewhere(t, to_owner(t).start)

    ready = 0
    for b in range(len(blocks)):
        along_rows(b)
        if b < len(aux):
            aux[b].start()
        if ready < last and blocks[b][0] >= sum(groups[ready][:2]):
            along_cols(ready)
            send(ready)
            ready += 1
    along_cols(last)
    send(last)

    for copy in aux:
        copy.wait()
    for l in range(levels):
        weight_ref[l] = 1.0 / (1.0 + jnp.exp(-(level[l] - pbl[...]) / RAMP_DEPTH))
    for j, (first, count, fold, tile) in enumerate(groups):
        scale = pick(
            [
                jnp.full((SUB, LANES), strength[f // variables, f % variables], F32)
                for f in range(first, first + count)
            ],
            lane_group(SUB) // fold,
        )
        for t in tiles_of(j):
            scale_ref[t * SUB:(t + 1) * SUB] = scale
    col_hi, col_lo = split(basis(
        cols * gy,
        (iy * cols + iota((LANES, cols), 1)).astype(F32),
        lax.rem(iota((LANES, cols), 0), KY).astype(F32),
    ))
    col_ref[...] = jnp.concatenate([col_hi, col_hi, col_lo], axis=0)
    row_hi, row_lo = split(basis(
        rows * gx,
        (ix * rows + iota((rows, 4 * KX), 0)).astype(F32),
        lax.rem(iota((rows, 4 * KX), 1), KX).astype(F32),
    ))
    row_ref[...] = jnp.where(
        iota((rows, 4 * KX), 1) < 2 * KX, row_hi.astype(F32), row_lo.astype(F32)
    ).astype(BF16)

    for k in range(n_owned):
        @pl.when(owns[k] > 0)
        def _(k=k):
            t = tile_at[k]
            settle(got.at[k], part_recv.at[k])
            full[t] = mine[t] + add_tiles(got, k)
            each_other(lambda target: to_all(t, group_at[k], target).start())

    def widen(j):
        first, count, fold, tile = groups[j]
        span = slice(tile * SUB, tile * SUB + KX // fold)
        hi, lo = expand_cols([(coef_ref[span] * scale_ref[span], count, fold)], col_ref[...])
        keep = wide_ref if j == early - 1 else wave.at[j % 2]
        keep[0, :count * KX] = hi
        keep[1, :count * KX] = lo

    def finish(j):
        first, count, fold, tile = groups[j]
        for k in range(count):
            f = first + k
            span = slice(k * KX, (k + 1) * KX)
            early_ref[f] = expand_rows(
                wave[j % 2, 0, span], wave[j % 2, 1, span], row_ref[...],
                weight_ref[f // variables],
            )

    def arrive(stage):
        here = [t for t in range(tiles) if group_of[t] == stage]
        held = [owners[t] for t in here]
        own = sum((owned(t).astype(jnp.int32) for t in here), jnp.int32(0))
        settle_tiles(
            full, full_recv.at[stage], here[0], len(here), own, max(held.count(o) for o in held)
        )
        for t in here:
            coef_ref[t * SUB:(t + 1) * SUB] = full[t]

    for j in range(early):
        arrive(j)
        widen(j)
        if j:
            finish(j - 1)
    arrive(early)
    settle_tiles(mine, part_send, 0, tiles, sum(owns), n_owned)
    for c in range(1, n_owned + 1):
        pl.when(sum(owns) == c)(lambda c=c: settle(got.at[pl.ds(0, c)], full_send))


def synthesis_kernel(
    tail, coef_ref, scale_ref, weight_ref, row_ref, col_ref, early_ref, wide_ref,
    tend_hbm, energy_hbm,
    tend, energy_ref, tend_sem, energy_sem,
):
    levels, variables = energy_ref.shape
    fields = levels * variables
    groups, tiles = plan_groups(fields)
    done, wide = groups[-tail - 1][:2]

    def out(first, count):
        level, at = first // variables, first % variables
        span = pl.ds(first - done, count) if first >= done else pl.ds(first, count)
        return pltpu.make_async_copy(
            (tend if first >= done else early_ref).at[span],
            tend_hbm.at[level, pl.ds(at, count)],
            tend_sem,
        )

    for first in range(0, done, variables):
        out(first, min(variables, done - first)).start()

    at_row = iota((levels, variables), 0)
    at_col = iota((levels, variables), 1)
    energy = jnp.zeros((levels, variables), F32)
    for first, count, fold, tile in groups:
        coef = coef_ref[tile * SUB:tile * SUB + KX // fold]
        power = jnp.sum(coef * coef, axis=0, keepdims=True)
        group = lane_group(1) // fold
        for k in range(count):
            f = first + k
            one = jnp.sum(jnp.where(group == k, power, 0.0), axis=(0, 1), keepdims=True)
            energy = jnp.where(
                (at_row == f // variables) & (at_col == f % variables), one, energy
            )
    energy_ref[...] = energy * (1.0 / (KX * KY))
    result = pltpu.make_async_copy(energy_ref, energy_hbm, energy_sem)
    result.start()

    parts = []
    for first, count, fold, tile in groups[-tail:]:
        span = slice(tile * SUB, tile * SUB + KX // fold)
        parts.append((coef_ref[span] * scale_ref[span], count, fold))
    hi, lo = expand_cols(parts, col_ref[...])
    for f in range(done, fields):
        k = f - done if f < done + wide else f - done - wide
        span = slice(k * KX, (k + 1) * KX)
        pair = (wide_ref[0, span], wide_ref[1, span]) if f < done + wide else (hi[span], lo[span])
        tend[f - done] = expand_rows(*pair, row_ref[...], weight_ref[f // variables])
        if f > done:
            out(f - 1, 1).start()
    out(fields - 1, 1).start()

    pltpu.make_async_copy(tend_hbm, tend_hbm, tend_sem).wait()
    result.wait()


def per_device(gx, gy, prognostic_values, forcing_host_values, strength, level_height, pbl_height):
    levels, variables, rows, cols = prognostic_values.shape
    fields = levels * variables
    n_dev = gx * gy
    groups, tiles = plan_groups(fields)
    n_owned = max(plan_owners(gx, gy, tiles)[1]) + 1
    tail = min(TAIL, len(groups) - 1)
    blocks = plan_blocks(fields)
    done = groups[-tail - 1][0]
    anywhere = pl.BlockSpec(memory_space=pl.ANY)
    vmem = pl.BlockSpec(memory_space=pltpu.VMEM)
    dma = pltpu.SemaphoreType.DMA
    held = pl.pallas_call(
        functools.partial(analysis_kernel, (gx, gy, tail)),
        out_shape=(
            pltpu.VMEM((tiles * SUB, LANES), F32),
            pltpu.VMEM((tiles * SUB, LANES), F32),
            pltpu.VMEM((levels, rows, cols), F32),
            pltpu.VMEM((rows, 4 * KX), BF16),
            pltpu.VMEM((3 * LANES, cols), BF16),
            pltpu.VMEM((max(done, 1), rows, cols), BF16),
            pltpu.VMEM((2, LANES, cols), BF16),
        ),
        in_specs=[anywhere] * 5,
        out_specs=(vmem,) * 7,
        scratch_shapes=[
            pltpu.SMEM((levels, variables), F32),
            pltpu.SMEM((levels,), F32),
            pltpu.VMEM((rows, cols), F32),
            pltpu.VMEM((fields, rows, cols), F32),
            pltpu.VMEM((fields, rows, cols), BF16),
            pltpu.VMEM((fields, KX, cols), F32),
            pltpu.VMEM((tiles, SUB, LANES), F32),
            pltpu.VMEM((n_owned, n_dev - 1, SUB, LANES), F32),
            pltpu.VMEM((tiles, SUB, LANES), F32),
            pltpu.VMEM((2, 2, LANES, cols), BF16),
            dma((max(len(blocks), 3), 1 + max(len(b) % 2 for b in blocks))),
            dma,
            dma((n_owned,)),
            dma,
            dma((len(groups) - tail + 1,)),
        ],
        compiler_params=pltpu.CompilerParams(collective_id=0, has_side_effects=True),
        name="analysis",
    )(
        prognostic_values.reshape(fields, rows, cols),
        forcing_host_values.reshape(fields, rows, cols),
        strength,
        level_height,
        pbl_height,
    )
    tendency, energy = pl.pallas_call(
        functools.partial(synthesis_kernel, tail),
        out_shape=(
            jax.ShapeDtypeStruct((levels, variables, rows, cols), BF16),
            jax.ShapeDtypeStruct((levels, variables), F32),
        ),
        in_specs=[vmem] * 7,
        out_specs=(anywhere, anywhere),
        scratch_shapes=[
            pltpu.VMEM((fields - done, rows, cols), BF16),
            pltpu.VMEM((levels, variables), F32),
            dma,
            dma,
        ],
        name="synthesis",
    )(*[pltpu.with_memory_space_constraint(x, pltpu.VMEM) for x in held])
    return tendency, energy


def solution(mesh):
    return jax.shard_map(
        functools.partial(per_device, mesh.shape["gx"], mesh.shape["gy"]),
        mesh=mesh,
        in_specs=(P(None, None, "gx", "gy"), P(None, None, "gx", "gy"), P(), P(), P("gx", "gy")),
        out_specs=(P(None, None, "gx", "gy"), P()),
        check_vma=False,
    )
```
